32 devices in a mesh: replica: 1 (over z), heads: 4 (over y), model: 8 (over x, core).
Axes of the slice: x: 4, y: 4, z: 1, core: 2. Of those that a mesh axis runs over, the one named last changes fastest.
The devices are a block of a 4x4x8 slice.
Arguments:
- tokens: bfloat16 [256, 8192], P('replica')
- w_query: bfloat16 [8192, 8192], P(None, ('heads', 'model'))
- w_key: bfloat16 [8192, 1024], replicated
- w_value: bfloat16 [8192, 1024], replicated
- w_out: bfloat16 [8192, 8192], P(('heads', 'model'))
- key_cache: bfloat16 [256, 8, 1024, 128], P(('replica', 'model'))
- value_cache: bfloat16 [256, 8, 1024, 128], P(('replica', 'model'))
- lengths: int32 [256], P(('replica', 'model'))
Outputs:
- output 1: bfloat16 [256, 8192], P('replica')
- output 2: bfloat16 [256, 8, 128], P(('replica', 'model'))
- output 3: bfloat16 [256, 8, 128], P(('replica', 'model'))
All inputs are finite; a program needn't handle non-finite values.
Results may differ from the reference program's by a relative error of at most 0.002.
Values are sent between devices in bfloat16 or wider.
A program may use at most 768 MiB of HBM per device.

```python
import jax
import jax.numpy as jnp
from jax import lax

D = 8192
QHEADS = 64
KVHEADS = 8
HEAD = 128
BATCH = 256
CONTEXT = 1024
GROUP_SIZE = QHEADS // KVHEADS
SCALE = HEAD ** -0.5


def draw_lengths(len_key):
    len_keys = jax.random.split(len_key, 2)
    lengths = jax.random.randint(len_keys[0], (BATCH,), 1, CONTEXT, dtype=jnp.int32)
    perm_order = jax.random.permutation(len_keys[1], BATCH)
    return lengths.at[perm_order[0]].set(CONTEXT - 1).at[perm_order[1]].set(1)


def setup_inputs(seed: int = 0, part: int = 0) -> dict:
    base_key = jax.random.key(seed)
    part_key = jax.random.fold_in(base_key, part)
    part_keys = jax.random.split(part_key, 3)
    weight_keys = jax.random.split(base_key, 4)
    query_cols = QHEADS * HEAD
    kv_cols = KVHEADS * HEAD
    tokens = jax.random.normal(part_keys[0], (BATCH, D), jnp.float32)
    w_query = jax.random.normal(weight_keys[0], (D, query_cols), jnp.float32) * D ** -0.5
    w_key = jax.random.normal(weight_keys[1], (D, kv_cols), jnp.float32) * (3.0 * D ** -0.5)
    w_value = jax.random.normal(weight_keys[2], (D, kv_cols), jnp.float32) * D ** -0.5
    w_out = jax.random.normal(weight_keys[3], (query_cols, D), jnp.float32) * query_cols ** -0.5
    key_cache = 3.0 * jax.random.normal(part_keys[1], (BATCH, KVHEADS, CONTEXT, HEAD), jnp.float32)
    value_cache = jax.random.normal(part_keys[2], (BATCH, KVHEADS, CONTEXT, HEAD), jnp.float32)
    lengths = draw_lengths(jax.random.fold_in(part_key, 3))
    return {
        "tokens": tokens.astype(jnp.bfloat16),
        "w_query": w_query.astype(jnp.bfloat16),
        "w_key": w_key.astype(jnp.bfloat16),
        "w_value": w_value.astype(jnp.bfloat16),
        "w_out": w_out.astype(jnp.bfloat16),
        "key_cache": key_cache.astype(jnp.bfloat16),
        "value_cache": value_cache.astype(jnp.bfloat16),
        "lengths": lengths,
    }


def reference(tokens, w_query, w_key, w_value, w_out, key_cache, value_cache, lengths):
    queries = jnp.dot(tokens, w_query, preferred_element_type=jnp.float32).astype(jnp.bfloat16)
    queries = queries.reshape(BATCH, KVHEADS, GROUP_SIZE, HEAD)
    key_new = jnp.dot(tokens, w_key, preferred_element_type=jnp.float32).astype(jnp.bfloat16)
    key_new = key_new.reshape(BATCH, KVHEADS, HEAD)
    value_new = jnp.dot(tokens, w_value, preferred_element_type=jnp.float32).astype(jnp.bfloat16)
    value_new = value_new.reshape(BATCH, KVHEADS, HEAD)

    def one_sequence(item):
        q_seq, key_seq, value_seq, key_last, value_last, seq_len = item
        q_wide = q_seq.astype(jnp.float32)
        scores = jnp.einsum("grd,gtd->grt", q_wide, key_seq.astype(jnp.float32)) * SCALE
        score_new = jnp.einsum("grd,gd->gr", q_wide, key_last.astype(jnp.float32)) * SCALE
        positions = jnp.arange(CONTEXT)
        scores = jnp.where(positions < seq_len, scores, -jnp.inf)
        score_max = jnp.maximum(jnp.max(scores, axis=-1), score_new)
        weights = jnp.exp(scores - score_max[..., None])
        weight_new = jnp.exp(score_new - score_max)
        denom_sum = jnp.sum(weights, axis=-1) + weight_new
        weighted_sum = jnp.einsum("grt,gtd->grd", weights.astype(jnp.bfloat16).astype(jnp.float32), value_seq.astype(jnp.float32))
        weighted_sum = weighted_sum + weight_new.astype(jnp.bfloat16).astype(jnp.float32)[..., None] * value_last.astype(jnp.float32)[:, None, :]
        return (weighted_sum / denom_sum[..., None]).astype(jnp.bfloat16)

    attended = lax.map(one_sequence, (queries, key_cache, value_cache, key_new, value_new, lengths))
    mixed_sum = jnp.dot(attended.reshape(BATCH, QHEADS * HEAD), w_out, preferred_element_type=jnp.float32)
    out_tokens = (tokens.astype(jnp.float32) + mixed_sum).astype(jnp.bfloat16)
    return (out_tokens, key_new, value_new)
```

```python
import functools

import jax
import jax.numpy as jnp
from jax import lax
from jax.experimental import pallas as pl
from jax.experimental.pallas import tpu as pltpu
from jax.sharding import PartitionSpec as P

MESH = pl.DeviceIdType.MESH
CHUNKS = 2
OFFSET = 2


def attend(queries, key_rows, value_rows, key_last, value_last, seq_len):
    score_scale = queries.shape[-1] ** -0.5
    scores = jnp.einsum("bgrd,bgtd->bgrt", queries, key_rows, preferred_element_type=jnp.float32) * score_scale
    score_new = jnp.einsum("bgrd,bgd->bgr", queries, key_last, preferred_element_type=jnp.float32) * score_scale
    positions = lax.broadcasted_iota(jnp.int32, (1, 1, 1, key_rows.shape[2]), 3)
    scores = jnp.where(positions < seq_len[:, None, None, None], scores, -jnp.inf)
    score_max = jnp.maximum(jnp.max(scores, axis=-1), score_new)
    weights = jnp.exp(scores - score_max[..., None])
    weight_new = jnp.exp(score_new - score_max)
    denom_sum = jnp.sum(weights, axis=-1) + weight_new
    weighted_sum = jnp.einsum("bgrt,bgtd->bgrd", weights.astype(jnp.bfloat16), value_rows, preferred_element_type=jnp.float32)
    weighted_sum = weighted_sum + weight_new.astype(jnp.bfloat16).astype(jnp.float32)[..., None] * value_last.astype(jnp.float32)[:, :, None, :]
    return (weighted_sum / denom_sum[..., None]).astype(jnp.bfloat16)


def mix_kernel(ny, nx, o_ref, wo_ref, tok_ref, out_ref,
               w_buf, o_all, part, recv1, recv2, tok_buf,
               o_send, o_recv, w_sem, tok_sem, sems1, sems2, sems3, sems4, sems_d):
    y = lax.axis_index("heads")
    model = lax.axis_index("model")
    x = lax.div(model, 2)
    core = lax.rem(model, 2)
    rows = o_ref.shape[1]
    depth = wo_ref.shape[0]
    cols = wo_ref.shape[1] // 2
    half = cols // 2
    block = half // 4
    r = rows // CHUNKS
    groups = 2 * nx

    def dev(yy, xx, cc):
        return {"heads": lax.rem(yy + ny, ny), "model": 2 * lax.rem(xx + nx, nx) + cc}

    partner = dev(y, x, 1 - core)
    x_next, x_prev = dev(y, x + 1, core), dev(y, x - 1, core)
    y_next, y_prev = dev(y + 1, x, core), dev(y - 1, x, core)

    barrier = pltpu.get_barrier_semaphore()
    peers = [partner, y_next, y_prev]
    for step in range(1, nx):
        for cc in range(2):
            peers.append(dev(y, x + step, cc))
    for peer in peers:
        pl.semaphore_signal(barrier, inc=1, device_id=peer, device_id_type=MESH)
    my_cols = pl.ds(pl.multiple_of(core * cols, cols), cols)
    other_cols = pl.ds(pl.multiple_of((1 - core) * cols, cols), cols)
    my_rows = pl.ds(pl.multiple_of(core * depth, depth), depth)
    own_w = pltpu.make_async_copy(wo_ref.at[:, my_cols], w_buf.at[my_rows], w_sem.at[2])
    own_w.start()
    pos1 = (x, y)
    pos2 = (y, x)
    tok_copies = []
    for h in range(2):
        c0 = pl.multiple_of(core * cols + h * half + pos1[h] * block, block)
        copy = pltpu.make_async_copy(tok_ref.at[pl.ds(2 * pos2[h], 2), :, pl.ds(c0, block)], tok_buf.at[h], tok_sem.at[h])
        copy.start()
        tok_copies.append(copy)
    pl.semaphore_wait(barrier, len(peers))

    o_copies = []
    n = 0
    for step in [1, nx - 1] + list(range(2, nx - 1)) + [0]:
        for cc in range(2):
            tx = lax.rem(x + step, nx)
            if step == 0:
                if cc == 1:
                    continue
                target = partner
            else:
                target = dev(y, x + step, cc)
            copy = pltpu.make_async_remote_copy(
                src_ref=o_ref.at[tx], dst_ref=o_all.at[model],
                send_sem=o_send.at[n],
                recv_sem=o_recv.at[(nx - step) % nx * 2 + core if step else 2 * 0],
                device_id=target, device_id_type=MESH)
            copy.start()
            o_copies.append(copy)
            n += 1
    w_copy = pltpu.make_async_remote_copy(
        src_ref=wo_ref.at[:, other_cols], dst_ref=w_buf.at[my_rows],
        send_sem=w_sem.at[0], recv_sem=w_sem.at[1], device_id=partner, device_id_type=MESH)
    w_copy.start()
    o_all[pl.ds(model, 1)] = o_ref[pl.ds(x, 1)]

    def wait_recv(dst, sem):
        pltpu.make_async_copy(dst, dst, sem).wait()

    for step in range(1, nx):
        for cc in range(2):
            source = 2 * lax.rem(x + step, nx) + cc
            wait_recv(o_all.at[source], o_recv.at[step * 2 + cc])
    wait_recv(o_all.at[2 * x + 1 - core], o_recv.at[0])
    own_w.wait()
    w_copy.wait_recv()
    for copy in tok_copies:
        copy.wait()

    sends = list(o_copies)

    def remote(src, dst, sems, index, target):
        copy = pltpu.make_async_remote_copy(
            src_ref=src, dst_ref=dst, send_sem=sems.at[0, index], recv_sem=sems.at[1, index],
            device_id=target, device_id_type=MESH)
        copy.start()
        sends.append(copy)
        return copy

    nexts = ((x_next, y_next), (y_next, x_next))
    prevs = ((x_prev, y_prev), (y_prev, x_prev))
    flows = {}
    hg = groups // 2

    def base(h):
        return h * half

    def cols_of(h, d):
        return pl.ds(pl.multiple_of(base(h) + lax.rem(d + 4, 4) * block, block), block)

    def compute(k, h, d):
        lhs = o_all[:, k * r:(k + 1) * r, :].reshape(groups * r, o_all.shape[2])
        acc = jnp.dot(lhs, w_buf[:, cols_of(h, d)], preferred_element_type=jnp.float32)
        part[k, :, :, cols_of(h, d)] = acc.reshape(groups, r, block)

    def sidx(k, h, i):
        return (k * 2 + h) * 6 + i

    def s0(k):
        for h in range(2):
            p = pos1[h]
            compute(k, h, p + 2)
            c = cols_of(h, p + 2)
            flows[k, h, 0] = remote(part.at[k, 0:hg, :, c], recv1.at[k, h, 0], sems1, sidx(k, h, 0), nexts[h][0])
            flows[k, h, 1] = remote(part.at[k, hg:groups, :, c], recv1.at[k, h, 1], sems1, sidx(k, h, 1), prevs[h][0])
        for h in range(2):
            p = pos1[h]
            compute(k, h, p + 1)
            flows[k, h, 2] = remote(part.at[k, hg:groups, :, cols_of(h, p + 1)], recv1.at[k, h, 2], sems1, sidx(k, h, 2), nexts[h][0])
            compute(k, h, p - 1)
            flows[k, h, 3] = remote(part.at[k, 0:hg, :, cols_of(h, p - 1)], recv1.at[k, h, 3], sems1, sidx(k, h, 3), prevs[h][0])
        for h in range(2):
            compute(k, h, pos1[h])

    def s1(k):
        for h in range(2):
            p = pos1[h]
            c = cols_of(h, p + 1)
            flows[k, h, 0].wait_recv()
            part[k, 0:hg, :, c] = part[k, 0:hg, :, c] + recv1[k, h, 0]
            flows[k, h, 4] = remote(part.at[k, 0:hg, :, c], recv1.at[k, h, 4], sems1, sidx(k, h, 4), nexts[h][0])
            c = cols_of(h, p - 1)
            flows[k, h, 1].wait_recv()
            part[k, hg:groups, :, c] = part[k, hg:groups, :, c] + recv1[k, h, 1]
            flows[k, h, 5] = remote(part.at[k, hg:groups, :, c], recv1.at[k, h, 5], sems1, sidx(k, h, 5), prevs[h][0])

    def s2(k):
        for h in range(2):
            c = cols_of(h, pos1[h])
            q = pos2[h]
            for i in (2, 3, 4, 5):
                flows[k, h, i].wait_recv()
            part[k, 0:hg, :, c] = part[k, 0:hg, :, c] + recv1[k, h, 3] + recv1[k, h, 4]
            part[k, hg:groups, :, c] = part[k, hg:groups, :, c] + recv1[k, h, 2] + recv1[k, h, 5]
            far, up, down = lax.rem(q + 2, 4), lax.rem(q + 1, 4), lax.rem(q + 3, 4)
            flows[k, h, 10] = remote(part.at[k, 2 * far, :, c], recv2.at[k, h, 0], sems2, sidx(k, h, 0), nexts[h][1])
            flows[k, h, 11] = remote(part.at[k, 2 * far + 1, :, c], recv2.at[k, h, 1], sems2, sidx(k, h, 1), prevs[h][1])
            flows[k, h, 12] = remote(part.at[k, 2 * up + 1, :, c], recv2.at[k, h, 2], sems2, sidx(k, h, 2), nexts[h][1])
            flows[k, h, 13] = remote(part.at[k, 2 * down, :, c], recv2.at[k, h, 3], sems2, sidx(k, h, 3), prevs[h][1])

    def s3(k):
        for h in range(2):
            c = cols_of(h, pos1[h])
            q = pos2[h]
            up, down = lax.rem(q + 1, 4), lax.rem(q + 3, 4)
            flows[k, h, 10].wait_recv()
            part[k, 2 * up, :, c] = part[k, 2 * up, :, c] + recv2[k, h, 0]
            flows[k, h, 14] = remote(part.at[k, 2 * up, :, c], recv2.at[k, h, 4], sems2, sidx(k, h, 4), nexts[h][1])
            flows[k, h, 11].wait_recv()
            part[k, 2 * down + 1, :, c] = part[k, 2 * down + 1, :, c] + recv2[k, h, 1]
            flows[k, h, 15] = remote(part.at[k, 2 * down + 1, :, c], recv2.at[k, h, 5], sems2, sidx(k, h, 5), prevs[h][1])

    def out_cols(h, d):
        return pl.ds(pl.multiple_of(core * cols + base(h) + lax.rem(d + 4, 4) * block, block), block)

    def region(k, g0, ng, c):
        return out_ref.at[pl.ds(g0, ng), k * r:(k + 1) * r, c]

    def aidx(k, h, i):
        return (k * 2 + h) * 4 + i

    def s4(k):
        for h in range(2):
            c = cols_of(h, pos1[h])
            oc = out_cols(h, pos1[h])
            q = pos2[h]
            for i in (12, 13, 14, 15):
                flows[k, h, i].wait_recv()
            low = part[k, 2 * q, :, c] + recv2[k, h, 3] + recv2[k, h, 4]
            high = part[k, 2 * q + 1, :, c] + recv2[k, h, 2] + recv2[k, h, 5]
            low = tok_buf[h, 0, k * r:(k + 1) * r, :].astype(jnp.float32) + low
            high = tok_buf[h, 1, k * r:(k + 1) * r, :].astype(jnp.float32) + high
            out_ref[2 * q, k * r:(k + 1) * r, oc] = low.astype(out_ref.dtype)
            out_ref[2 * q + 1, k * r:(k + 1) * r, oc] = high.astype(out_ref.dtype)
            src = region(k, 2 * q, 2, oc)
            flows[k, h, 20] = remote(src, src, sems3, aidx(k, h, 0), nexts[h][1])
            flows[k, h, 21] = remote(src, src, sems3, aidx(k, h, 1), prevs[h][1])

    def s5(k):
        for h in range(2):
            oc = out_cols(h, pos1[h])
            q = pos2[h]
            up, down = lax.rem(q + 1, 4), lax.rem(q + 3, 4)
            wait_recv(region(k, 2 * down, 2, oc), sems3.at[1, aidx(k, h, 0)])
            src = region(k, 2 * down, 1, oc)
            flows[k, h, 22] = remote(src, src, sems3, aidx(k, h, 2), nexts[h][1])
            wait_recv(region(k, 2 * up, 2, oc), sems3.at[1, aidx(k, h, 1)])
            src = region(k, 2 * up + 1, 1, oc)
            flows[k, h, 23] = remote(src, src, sems3, aidx(k, h, 3), prevs[h][1])

    def didx(k, h, i):
        return (k * 2 + h) * 5 + i

    def s6(k):
        for h in range(2):
            oc = out_cols(h, pos1[h])
            q = pos2[h]
            far = lax.rem(q + 2, 4)
            wait_recv(region(k, 2 * far, 1, oc), sems3.at[1, aidx(k, h, 2)])
            wait_recv(region(k, 2 * far + 1, 1, oc), sems3.at[1, aidx(k, h, 3)])
            src = region(k, 0, groups, oc)
            flows[k, h, 30] = remote(src, src, sems4, aidx(k, h, 0), nexts[h][0])
            flows[k, h, 31] = remote(src, src, sems4, aidx(k, h, 1), prevs[h][0])
            remote(src, src, sems_d, didx(k, h, 0), partner)

    def s7(k):
        for h in range(2):
            p = pos1[h]
            down, up = out_cols(h, p - 1), out_cols(h, p + 1)
            wait_recv(region(k, 0, groups, down), sems4.at[1, aidx(k, h, 0)])
            src = region(k, 0, hg, down)
            remote(src, src, sems4, aidx(k, h, 2), nexts[h][0])
            wait_recv(region(k, 0, groups, up), sems4.at[1, aidx(k, h, 1)])
            src = region(k, hg, hg, up)
            remote(src, src, sems4, aidx(k, h, 3), prevs[h][0])
            src = region(k, 0, groups, down)
            remote(src, src, sems_d, didx(k, h, 1), partner)
            src = region(k, 0, groups, up)
            remote(src, src, sems_d, didx(k, h, 2), partner)

    def s8(k):
        for h in range(2):
            far = out_cols(h, pos1[h] + 2)
            for i in range(2):
                src = region(k, i * hg, hg, far)
                wait_recv(src, sems4.at[1, aidx(k, h, 2 + i)])
                remote(src, src, sems_d, didx(k, h, 3 + i), partner)

    stages = [s0, s1, s2, s3, s4, s5, s6, s7, s8]
    for slot in range(len(stages) + OFFSET * (CHUNKS - 1)):
        for k in range(CHUNKS):
            if 0 <= slot - OFFSET * k < len(stages):
                stages[slot - OFFSET * k](k)

    def other_out_cols(h, d):
        return pl.ds(pl.multiple_of((1 - core) * cols + base(h) + lax.rem(d + 4, 4) * block, block), block)

    for k in range(CHUNKS):
        for h in range(2):
            p = pos1[h]
            wait_recv(region(k, 0, groups, other_out_cols(h, p)), sems_d.at[1, didx(k, h, 0)])
            wait_recv(region(k, 0, groups, other_out_cols(h, p - 1)), sems_d.at[1, didx(k, h, 1)])
            wait_recv(region(k, 0, groups, other_out_cols(h, p + 1)), sems_d.at[1, didx(k, h, 2)])
            for i in range(2):
                wait_recv(region(k, i * hg, hg, other_out_cols(h, p + 2)), sems_d.at[1, didx(k, h, 3 + i)])
    for copy in sends:
        copy.wait_send()
    w_copy.wait_send()


def mix(ny, nx, o_parts, w_out, tokens):
    groups = 2 * nx
    rows = o_parts.shape[1]
    width = w_out.shape[1]
    cols = width // 2
    block = cols // 8
    r = rows // CHUNKS
    any_spec = pl.BlockSpec(memory_space=pl.ANY)
    vmem_spec = pl.BlockSpec(memory_space=pltpu.VMEM)
    dma = pltpu.SemaphoreType.DMA
    return pl.pallas_call(
        functools.partial(mix_kernel, ny, nx),
        out_shape=jax.ShapeDtypeStruct((groups, rows, width), jnp.bfloat16),
        in_specs=[vmem_spec, any_spec, any_spec],
        out_specs=vmem_spec,
        scratch_shapes=[
            pltpu.VMEM((2 * w_out.shape[0], cols), jnp.bfloat16),
            pltpu.VMEM((groups, rows, 2 * w_out.shape[0]), jnp.bfloat16),
            pltpu.VMEM((CHUNKS, groups, r, cols), jnp.float32),
            pltpu.VMEM((CHUNKS, 2, 6, groups // 2, r, block), jnp.float32),
            pltpu.VMEM((CHUNKS, 2, 6, r, block), jnp.float32),
            pltpu.VMEM((2, 2, rows, block), jnp.bfloat16),
            dma((2 * nx,)), dma((2 * nx,)), dma((3,)), dma((2,)),
            dma((2, CHUNKS * 12)), dma((2, CHUNKS * 12)), dma((2, CHUNKS * 8)), dma((2, CHUNKS * 8)), dma((2, CHUNKS * 10)),
        ],
        compiler_params=pltpu.CompilerParams(collective_id=3, has_side_effects=True, vmem_limit_bytes=48 * 1024 * 1024),
        name="mix",
    )(o_parts, w_out, tokens.reshape(groups, rows, width))


def solution(mesh):
    heads_count = mesh.shape["heads"]
    model_count = mesh.shape["model"]

    def local_step(tokens, w_query, w_key, w_value, w_out, key_cache, value_cache, lengths):
        batch_all = tokens.shape[0]
        local_rows = key_cache.shape[0]
        kv_count = key_cache.shape[1]
        head_dim = key_cache.shape[3]
        heads_local = w_query.shape[1] // head_dim
        heads_shard = heads_local * model_count
        group_size = heads_shard * heads_count // kv_count
        shard_groups = max(1, heads_shard // group_size)
        head_index = lax.axis_index("heads")
        model_index = lax.axis_index("model")
        queries = jnp.dot(tokens, w_query, preferred_element_type=jnp.float32).astype(jnp.bfloat16)
        queries = lax.all_to_all(queries.reshape(batch_all, heads_local, head_dim), "model", 0, 1, tiled=True)
        own_tokens = lax.dynamic_slice_in_dim(tokens, model_index * local_rows, local_rows, 0)
        key_new = jnp.dot(own_tokens, w_key, preferred_element_type=jnp.float32).astype(jnp.bfloat16)
        key_new = key_new.reshape(local_rows, kv_count, head_dim)
        value_new = jnp.dot(own_tokens, w_value, preferred_element_type=jnp.float32).astype(jnp.bfloat16)
        value_new = value_new.reshape(local_rows, kv_count, head_dim)
        first_group = head_index * heads_shard // group_size
        attended = attend(
            queries.reshape(local_rows, shard_groups, heads_shard // shard_groups, head_dim),
            lax.dynamic_slice_in_dim(key_cache, first_group, shard_groups, 1),
            lax.dynamic_slice_in_dim(value_cache, first_group, shard_groups, 1),
            lax.dynamic_slice_in_dim(key_new, first_group, shard_groups, 1),
            lax.dynamic_slice_in_dim(value_new, first_group, shard_groups, 1),
            lengths,
        )
        chips = model_count // 2
        o_parts = attended.reshape(local_rows, chips, heads_shard // chips * head_dim).transpose(1, 0, 2)
        out_tokens = mix(heads_count, chips, o_parts, w_out, tokens).reshape(tokens.shape)
        return (out_tokens, key_new, value_new)

    cache_spec = P(("replica", "model"), None, None, None)
    new_spec = P(("replica", "model"), None, None)
    return jax.shard_map(
        local_step,
        mesh=mesh,
        in_specs=(P("replica", None), P(None, ("heads", "model")), P(None, None), P(None, None), P(("heads", "model"), None), cache_spec, cache_spec, P(("replica", "model"))),
        out_specs=(P("replica", None), new_spec, new_spec),
        check_vma=False,
    )
```

```python
import functools

import jax
import jax.numpy as jnp
from jax import lax
from jax.experimental import pallas as pl
from jax.experimental.pallas import tpu as pltpu
from jax.sharding import PartitionSpec as P

MESH = pl.DeviceIdType.MESH
CHUNKS = 1
OFFSET = 1
CHUNK_K = 8
SLOTS = 8
SEQS = 2


def mix_kernel(ny, nx, o_ref, wo_ref, tok_ref, out_ref,
               w_buf, o_all, part, recv1, recv2, tok_buf,
               o_send, o_recv, w_sem, tok_sem, sems1, sems2, sems3, sems4, sems_d):
    y = lax.axis_index("heads")
    model = lax.axis_index("model")
    x = lax.div(model, 2)
    core = lax.rem(model, 2)
    rows = o_ref.shape[1]
    depth = wo_ref.shape[0]
    cols = wo_ref.shape[1] // 2
    half = cols // 2
    block = half // 4
    r = rows // CHUNKS
    groups = 2 * nx

    def dev(yy, xx, cc):
        return {"heads": lax.rem(yy + ny, ny), "model": 2 * lax.rem(xx + nx, nx) + cc}

    partner = dev(y, x, 1 - core)
    x_next, x_prev = dev(y, x + 1, core), dev(y, x - 1, core)
    y_next, y_prev = dev(y + 1, x, core), dev(y - 1, x, core)

    barrier = pltpu.get_barrier_semaphore()
    peers = [partner, y_next, y_prev]
    for step in range(1, nx):
        for cc in range(2):
            peers.append(dev(y, x + step, cc))
    for peer in peers:
        pl.semaphore_signal(barrier, inc=1, device_id=peer, device_id_type=MESH)
    my_cols = pl.ds(pl.multiple_of(core * cols, cols), cols)
    other_cols = pl.ds(pl.multiple_of((1 - core) * cols, cols), cols)
    my_rows = pl.ds(pl.multiple_of(core * depth, depth), depth)
    own_w = pltpu.make_async_copy(wo_ref.at[:, my_cols], w_buf.at[my_rows], w_sem.at[2])
    own_w.start()
    pos1 = (x, y)
    pos2 = (y, x)
    tok_copies = []
    for h in range(2):
        c0 = pl.multiple_of(core * cols + h * half + pos1[h] * block, block)
        copy = pltpu.make_async_copy(tok_ref.at[pl.ds(2 * pos2[h], 2), :, pl.ds(c0, block)], tok_buf.at[h], tok_sem.at[h])
        copy.start()
        tok_copies.append(copy)
    pl.semaphore_wait(barrier, len(peers))

    o_copies = []
    n = 0
    for step in [1, nx - 1] + list(range(2, nx - 1)) + [0]:
        for cc in range(2):
            tx = lax.rem(x + step, nx)
            if step == 0:
                if cc == 1:
                    continue
                target = partner
            else:
                target = dev(y, x + step, cc)
            copy = pltpu.make_async_remote_copy(
                src_ref=o_ref.at[tx], dst_ref=o_all.at[model],
                send_sem=o_send.at[n],
                recv_sem=o_recv.at[(nx - step) % nx * 2 + core if step else 2 * 0],
                device_id=target, device_id_type=MESH)
            copy.start()
            o_copies.append(copy)
            n += 1
    w_copy = pltpu.make_async_remote_copy(
        src_ref=wo_ref.at[:, other_cols], dst_ref=w_buf.at[my_rows],
        send_sem=w_sem.at[0], recv_sem=w_sem.at[1], device_id=partner, device_id_type=MESH)
    w_copy.start()
    o_all[pl.ds(model, 1)] = o_ref[pl.ds(x, 1)]

    def wait_recv(dst, sem):
        pltpu.make_async_copy(dst, dst, sem).wait()

    for step in range(1, nx):
        for cc in range(2):
            source = 2 * lax.rem(x + step, nx) + cc
            wait_recv(o_all.at[source], o_recv.at[step * 2 + cc])
    wait_recv(o_all.at[2 * x + 1 - core], o_recv.at[0])
    own_w.wait()
    w_copy.wait_recv()
    for copy in tok_copies:
        copy.wait()

    sends = list(o_copies)

    def remote(src, dst, sems, index, target):
        copy = pltpu.make_async_remote_copy(
            src_ref=src, dst_ref=dst, send_sem=sems.at[0, index], recv_sem=sems.at[1, index],
            device_id=target, device_id_type=MESH)
        copy.start()
        sends.append(copy)
        return copy

    nexts = ((x_next, y_next), (y_next, x_next))
    prevs = ((x_prev, y_prev), (y_prev, x_prev))
    flows = {}
    hg = groups // 2

    def base(h):
        return h * half

    def cols_of(h, d):
        return pl.ds(pl.multiple_of(base(h) + lax.rem(d + 4, 4) * block, block), block)

    def compute(k, h, d):
        lhs = o_all[:, k * r:(k + 1) * r, :].reshape(groups * r, o_all.shape[2])
        acc = jnp.dot(lhs, w_buf[:, cols_of(h, d)], preferred_element_type=jnp.float32)
        part[k, :, :, cols_of(h, d)] = acc.reshape(groups, r, block)

    def sidx(k, h, i):
        return (k * 2 + h) * 6 + i

    def s0(k):
        for h in range(2):
            p = pos1[h]
            compute(k, h, p + 2)
            c = cols_of(h, p + 2)
            flows[k, h, 0] = remote(part.at[k, 0:hg, :, c], recv1.at[k, h, 0], sems1, sidx(k, h, 0), nexts[h][0])
            flows[k, h, 1] = remote(part.at[k, hg:groups, :, c], recv1.at[k, h, 1], sems1, sidx(k, h, 1), prevs[h][0])
        for h in range(2):
            p = pos1[h]
            compute(k, h, p + 1)
            flows[k, h, 2] = remote(part.at[k, hg:groups, :, cols_of(h, p + 1)], recv1.at[k, h, 2], sems1, sidx(k, h, 2), nexts[h][0])
            compute(k, h, p - 1)
            flows[k, h, 3] = remote(part.at[k, 0:hg, :, cols_of(h, p - 1)], recv1.at[k, h, 3], sems1, sidx(k, h, 3), prevs[h][0])
        for h in range(2):
            compute(k, h, pos1[h])

    def s1(k):
        for h in range(2):
            p = pos1[h]
            c = cols_of(h, p + 1)
            flows[k, h, 0].wait_recv()
            part[k, 0:hg, :, c] = part[k, 0:hg, :, c] + recv1[k, h, 0]
            flows[k, h, 4] = remote(part.at[k, 0:hg, :, c], recv1.at[k, h, 4], sems1, sidx(k, h, 4), nexts[h][0])
            c = cols_of(h, p - 1)
            flows[k, h, 1].wait_recv()
            part[k, hg:groups, :, c] = part[k, hg:groups, :, c] + recv1[k, h, 1]
            flows[k, h, 5] = remote(part.at[k, hg:groups, :, c], recv1.at[k, h, 5], sems1, sidx(k, h, 5), prevs[h][0])

    def s2(k):
        for h in range(2):
            c = cols_of(h, pos1[h])
            q = pos2[h]
            for i in (2, 3, 4, 5):
                flows[k, h, i].wait_recv()
            part[k, 0:hg, :, c] = part[k, 0:hg, :, c] + recv1[k, h, 3] + recv1[k, h, 4]
            part[k, hg:groups, :, c] = part[k, hg:groups, :, c] + recv1[k, h, 2] + recv1[k, h, 5]
            far, up, down = lax.rem(q + 2, 4), lax.rem(q + 1, 4), lax.rem(q + 3, 4)
            flows[k, h, 10] = remote(part.at[k, 2 * far, :, c], recv2.at[k, h, 0], sems2, sidx(k, h, 0), nexts[h][1])
            flows[k, h, 11] = remote(part.at[k, 2 * far + 1, :, c], recv2.at[k, h, 1], sems2, sidx(k, h, 1), prevs[h][1])
            flows[k, h, 12] = remote(part.at[k, 2 * up + 1, :, c], recv2.at[k, h, 2], sems2, sidx(k, h, 2), nexts[h][1])
            flows[k, h, 13] = remote(part.at[k, 2 * down, :, c], recv2.at[k, h, 3], sems2, sidx(k, h, 3), prevs[h][1])

    def s3(k):
        for h in range(2):
            c = cols_of(h, pos1[h])
            q = pos2[h]
            up, down = lax.rem(q + 1, 4), lax.rem(q + 3, 4)
            flows[k, h, 10].wait_recv()
            part[k, 2 * up, :, c] = part[k, 2 * up, :, c] + recv2[k, h, 0]
            flows[k, h, 14] = remote(part.at[k, 2 * up, :, c], recv2.at[k, h, 4], sems2, sidx(k, h, 4), nexts[h][1])
            flows[k, h, 11].wait_recv()
            part[k, 2 * down + 1, :, c] = part[k, 2 * down + 1, :, c] + recv2[k, h, 1]
            flows[k, h, 15] = remote(part.at[k, 2 * down + 1, :, c], recv2.at[k, h, 5], sems2, sidx(k, h, 5), prevs[h][1])

    def out_cols(h, d):
        return pl.ds(pl.multiple_of(core * cols + base(h) + lax.rem(d + 4, 4) * block, block), block)

    def region(k, g0, ng, c):
        return out_ref.at[pl.ds(g0, ng), k * r:(k + 1) * r, c]

    def aidx(k, h, i):
        return (k * 2 + h) * 4 + i

    def s4(k):
        for h in range(2):
            c = cols_of(h, pos1[h])
            oc = out_cols(h, pos1[h])
            q = pos2[h]
            for i in (12, 13, 14, 15):
                flows[k, h, i].wait_recv()
            low = part[k, 2 * q, :, c] + recv2[k, h, 3] + recv2[k, h, 4]
            high = part[k, 2 * q + 1, :, c] + recv2[k, h, 2] + recv2[k, h, 5]
            low = tok_buf[h, 0, k * r:(k + 1) * r, :].astype(jnp.float32) + low
            high = tok_buf[h, 1, k * r:(k + 1) * r, :].astype(jnp.float32) + high
            out_ref[2 * q, k * r:(k + 1) * r, oc] = low.astype(out_ref.dtype)
            out_ref[2 * q + 1, k * r:(k + 1) * r, oc] = high.astype(out_ref.dtype)
            src = region(k, 2 * q, 2, oc)
            flows[k, h, 20] = remote(src, src, sems3, aidx(k, h, 0), nexts[h][1])
            flows[k, h, 21] = remote(src, src, sems3, aidx(k, h, 1), prevs[h][1])

    def s5(k):
        for h in range(2):
            oc = out_cols(h, pos1[h])
            q = pos2[h]
            up, down = lax.rem(q + 1, 4), lax.rem(q + 3, 4)
            wait_recv(region(k, 2 * down, 2, oc), sems3.at[1, aidx(k, h, 0)])
            src = region(k, 2 * down, 1, oc)
            flows[k, h, 22] = remote(src, src, sems3, aidx(k, h, 2), nexts[h][1])
            wait_recv(region(k, 2 * up, 2, oc), sems3.at[1, aidx(k, h, 1)])
            src = region(k, 2 * up + 1, 1, oc)
            flows[k, h, 23] = remote(src, src, sems3, aidx(k, h, 3), prevs[h][1])

    def didx(k, h, i):
        return (k * 2 + h) * 5 + i

    def s6(k):
        for h in range(2):
            oc = out_cols(h, pos1[h])
            q = pos2[h]
            far = lax.rem(q + 2, 4)
            wait_recv(region(k, 2 * far, 1, oc), sems3.at[1, aidx(k, h, 2)])
            wait_recv(region(k, 2 * far + 1, 1, oc), sems3.at[1, aidx(k, h, 3)])
            src = region(k, 0, groups, oc)
            flows[k, h, 30] = remote(src, src, sems4, aidx(k, h, 0), nexts[h][0])
            flows[k, h, 31] = remote(src, src, sems4, aidx(k, h, 1), prevs[h][0])
            remote(src, src, sems_d, didx(k, h, 0), partner)

    def s7(k):
        for h in range(2):
            p = pos1[h]
            down, up = out_cols(h, p - 1), out_cols(h, p + 1)
            wait_recv(region(k, 0, groups, down), sems4.at[1, aidx(k, h, 0)])
            src = region(k, 0, hg, down)
            remote(src, src, sems4, aidx(k, h, 2), nexts[h][0])
            wait_recv(region(k, 0, groups, up), sems4.at[1, aidx(k, h, 1)])
            src = region(k, hg, hg, up)
            remote(src, src, sems4, aidx(k, h, 3), prevs[h][0])
            src = region(k, 0, groups, down)
            remote(src, src, sems_d, didx(k, h, 1), partner)
            src = region(k, 0, groups, up)
            remote(src, src, sems_d, didx(k, h, 2), partner)

    def s8(k):
        for h in range(2):
            far = out_cols(h, pos1[h] + 2)
            for i in range(2):
                src = region(k, i * hg, hg, far)
                wait_recv(src, sems4.at[1, aidx(k, h, 2 + i)])
                remote(src, src, sems_d, didx(k, h, 3 + i), partner)

    stages = [s0, s1, s2, s3, s4, s5, s6, s7, s8]
    for slot in range(len(stages) + OFFSET * (CHUNKS - 1)):
        for k in range(CHUNKS):
            if 0 <= slot - OFFSET * k < len(stages):
                stages[slot - OFFSET * k](k)

    def other_out_cols(h, d):
        return pl.ds(pl.multiple_of((1 - core) * cols + base(h) + lax.rem(d + 4, 4) * block, block), block)

    for k in range(CHUNKS):
        for h in range(2):
            p = pos1[h]
            wait_recv(region(k, 0, groups, other_out_cols(h, p)), sems_d.at[1, didx(k, h, 0)])
            wait_recv(region(k, 0, groups, other_out_cols(h, p - 1)), sems_d.at[1, didx(k, h, 1)])
            wait_recv(region(k, 0, groups, other_out_cols(h, p + 1)), sems_d.at[1, didx(k, h, 2)])
            for i in range(2):
                wait_recv(region(k, i * hg, hg, other_out_cols(h, p + 2)), sems_d.at[1, didx(k, h, 3 + i)])
    for copy in sends:
        copy.wait_send()
    w_copy.wait_send()


def mix(ny, nx, o_parts, w_out, tokens):
    groups = 2 * nx
    rows = o_parts.shape[1]
    width = w_out.shape[1]
    cols = width // 2
    block = cols // 8
    r = rows // CHUNKS
    any_spec = pl.BlockSpec(memory_space=pl.ANY)
    vmem_spec = pl.BlockSpec(memory_space=pltpu.VMEM)
    dma = pltpu.SemaphoreType.DMA
    return pl.pallas_call(
        functools.partial(mix_kernel, ny, nx),
        out_shape=jax.ShapeDtypeStruct((groups, rows, width), jnp.bfloat16),
        in_specs=[vmem_spec, any_spec, any_spec],
        out_specs=vmem_spec,
        scratch_shapes=[
            pltpu.VMEM((2 * w_out.shape[0], cols), jnp.bfloat16),
            pltpu.VMEM((groups, rows, 2 * w_out.shape[0]), jnp.bfloat16),
            pltpu.VMEM((CHUNKS, groups, r, cols), jnp.float32),
            pltpu.VMEM((CHUNKS, 2, 6, groups // 2, r, block), jnp.float32),
            pltpu.VMEM((CHUNKS, 2, 6, r, block), jnp.float32),
            pltpu.VMEM((2, 2, rows, block), jnp.bfloat16),
            dma((2 * nx,)), dma((2 * nx,)), dma((3,)), dma((2,)),
            dma((2, CHUNKS * 12)), dma((2, CHUNKS * 12)), dma((2, CHUNKS * 8)), dma((2, CHUNKS * 8)), dma((2, CHUNKS * 10)),
        ],
        compiler_params=pltpu.CompilerParams(collective_id=3, has_side_effects=True, vmem_limit_bytes=48 * 1024 * 1024),
        name="mix",
    )(o_parts, w_out, tokens.reshape(groups, rows, width))


def front_kernel(ny, nx, tok_ref, wq_ref, wk_ref, wv_ref, kc_ref, vc_ref, len_ref,
                 o_ref, kn_ref, vn_ref,
                 x_buf, wq_buf, wkv_buf, acc_q, acc_kv, q_send, q_recv, q_rows, kv_send, kv_all, kv_rows, kn_rows, o_rows, k_buf, v_buf,
                 x_sem, wq_sem, wk_sem, wv_sem, k_sem, v_sem, q_ss, q_rs, kv_ss, kv_rs):
    y = lax.axis_index("heads")
    model = lax.axis_index("model")
    nm = 2 * nx
    batch, width = x_buf.shape
    rows = batch // nm
    kc = width // CHUNK_K
    head = kc_ref.shape[3]
    context = kc_ref.shape[2]
    groups = kc_ref.shape[1] // ny
    kv_cols = groups * head
    heads = nm * (wq_ref.shape[1] // head)
    per_group = heads // groups
    hl = wq_ref.shape[1] // head

    def dev(yy, mm):
        return {"heads": lax.rem(yy + ny, ny), "model": lax.rem(mm + nm, nm)}

    barrier = pltpu.get_barrier_semaphore()
    peers = [dev(y, model + s) for s in range(1, nm)] + [dev(y + s, model) for s in range(1, ny)]
    for peer in peers:
        pl.semaphore_signal(barrier, inc=1, device_id=peer, device_id_type=MESH)

    copies = {}
    my_cols = pl.ds(pl.multiple_of(y * kv_cols, kv_cols), kv_cols)
    for i in range(CHUNK_K):
        ks = pl.ds(i * kc, kc)
        copies["x", i] = pltpu.make_async_copy(tok_ref.at[:, ks], x_buf.at[:, ks], x_sem.at[i])
        copies["q", i] = pltpu.make_async_copy(wq_ref.at[ks], wq_buf.at[ks], wq_sem.at[i])
        copies["x", i].start()
        copies["q", i].start()
    for i in range(CHUNK_K):
        ks = pl.ds(i * kc, kc)
        copies["k", i] = pltpu.make_async_copy(wk_ref.at[ks, my_cols], wkv_buf.at[ks, 0:kv_cols], wk_sem.at[i])
        copies["v", i] = pltpu.make_async_copy(wv_ref.at[ks, my_cols], wkv_buf.at[ks, kv_cols:2 * kv_cols], wv_sem.at[i])
        copies["k", i].start()
        copies["v", i].start()

    def cache_copies(b, slot):
        gs = pl.ds(y * groups, groups)
        return (pltpu.make_async_copy(kc_ref.at[b, gs], k_buf.at[slot], k_sem.at[slot]),
                pltpu.make_async_copy(vc_ref.at[b, gs], v_buf.at[slot], v_sem.at[slot]))

    for b in range(SLOTS):
        for copy in cache_copies(b, b):
            copy.start()

    for i in range(CHUNK_K):
        ks = pl.ds(i * kc, kc)
        copies["x", i].wait()
        copies["q", i].wait()
        prod = jnp.dot(x_buf[:, ks], wq_buf[ks, :], preferred_element_type=jnp.float32)
        acc_q[...] = prod if i == 0 else acc_q[...] + prod
    q_send[...] = acc_q[...].astype(jnp.bfloat16).reshape(nm, rows, hl * head)
    pl.semaphore_wait(barrier, len(peers))
    sends = []
    for n, s in enumerate((1, 7, 2, 6, 3, 5, 4)):
        target = lax.rem(model + s, nm)
        copy = pltpu.make_async_remote_copy(src_ref=q_send.at[target], dst_ref=q_recv.at[model], send_sem=q_ss.at[s],
                                            recv_sem=q_rs.at[nm - s], device_id=dev(y, target), device_id_type=MESH)
        copy.start()
        sends.append(copy)
    q_recv[pl.ds(model, 1)] = q_send[pl.ds(model, 1)]

    mine = pl.ds(pl.multiple_of(model * rows, rows), rows)
    for i in range(CHUNK_K):
        ks = pl.ds(i * kc, kc)
        copies["k", i].wait()
        copies["v", i].wait()
        prod = jnp.dot(x_buf[mine, ks], wkv_buf[ks, :], preferred_element_type=jnp.float32)
        acc_kv[...] = prod if i == 0 else acc_kv[...] + prod
    kv_bf = acc_kv[...].astype(jnp.bfloat16)
    kv_send[...] = kv_bf
    kv_all[pl.ds(y, 1)] = kv_bf[None]
    for j in range(2 * groups):
        kv_rows[j] = kv_bf[:, j * head:(j + 1) * head].astype(jnp.float32)
    for s in (1, 3, 2):
        copy = pltpu.make_async_remote_copy(src_ref=kv_send, dst_ref=kv_all.at[y], send_sem=kv_ss.at[s],
                                            recv_sem=kv_rs.at[ny - s], device_id=dev(y + s, model), device_id_type=MESH)
        copy.start()
        sends.append(copy)

    def arrive(dst, sem):
        pltpu.make_async_copy(dst, dst, sem).wait()

    for s in range(1, nm):
        arrive(q_recv.at[lax.rem(model + s, nm)], q_rs.at[s])
    for src in range(nm):
        for j in range(hl):
            q_rows[pl.ds(src * hl + j, rows, stride=heads), :] = q_recv[src, :, j * head:(j + 1) * head].astype(jnp.float32)

    scale = head ** -0.5
    positions = lax.broadcasted_iota(jnp.int32, (per_group, context), 1)

    def step(n, carry):
        pairs = []
        scores = []
        news = []
        for u in range(SEQS):
            b = n * SEQS + u
            slot = lax.rem(b, SLOTS)
            for copy in cache_copies(b, slot):
                copy.wait()
            length = len_ref[b]
            for g in range(groups):
                q = q_rows[pl.ds(pl.multiple_of(b * heads + g * per_group, per_group), per_group), :]
                s = lax.dot_general(q.astype(jnp.bfloat16), k_buf[slot, g], (((1,), (1,)), ((), ())), preferred_element_type=jnp.float32) * scale
                s = jnp.where(positions < length, s, -jnp.inf)
                k_last = kv_rows[g, pl.ds(b, 1), :]
                s_new = jnp.sum(q * k_last, axis=1, keepdims=True) * scale
                pairs.append((b, slot, g))
                scores.append(s)
                news.append(s_new)
        tops = [jnp.maximum(jnp.max(s, axis=1, keepdims=True), s_new) for s, s_new in zip(scores, news)]
        weights = [jnp.exp(s - m) for s, m in zip(scores, tops)]
        weight_news = [jnp.exp(s_new - m) for s_new, m in zip(news, tops)]
        sums = [jnp.sum(e, axis=1, keepdims=True) + e_new for e, e_new in zip(weights, weight_news)]
        for (b, slot, g), e, e_new, l in zip(pairs, weights, weight_news, sums):
            out = jnp.dot(e.astype(jnp.bfloat16), v_buf[slot, g], preferred_element_type=jnp.float32)
            v_last = kv_rows[groups + g, pl.ds(b, 1), :]
            out = out + e_new.astype(jnp.bfloat16).astype(jnp.float32) * v_last
            o_rows[pl.ds(pl.multiple_of(b * heads + g * per_group, per_group), per_group), :] = out / l
        for u in range(SEQS):
            b = n * SEQS + u

            @pl.when(b + SLOTS < rows)
            def _():
                for copy in cache_copies(b + SLOTS, lax.rem(b, SLOTS)):
                    copy.start()
        return carry

    lax.fori_loop(0, rows // SEQS, step, 0)
    hc = heads // nx
    for h in range(heads):
        o_ref[h // hc, :, (h % hc) * head:(h % hc + 1) * head] = o_rows[pl.ds(h, rows, stride=heads), :].astype(jnp.bfloat16)

    for s in range(1, ny):
        arrive(kv_all.at[lax.rem(y + s, ny)], kv_rs.at[s])
    kv_heads = ny * groups
    for part, ref in ((0, kn_ref), (1, vn_ref)):
        for g in range(kv_heads):
            c0 = part * kv_cols + (g % groups) * head
            kn_rows[part, pl.ds(g, rows, stride=kv_heads), :] = kv_all[g // groups, :, c0:c0 + head].astype(jnp.float32)
        ref[...] = kn_rows[part].reshape(rows, kv_heads, head).astype(jnp.bfloat16)
    for copy in sends:
        copy.wait_send()


def front(ny, nx, tokens, w_query, w_key, w_value, key_cache, value_cache, lengths):
    batch, width = tokens.shape
    rows, kv_heads, context, head = key_cache.shape
    nm = 2 * nx
    groups = kv_heads // ny
    kv_cols = groups * head
    heads = nm * w_query.shape[1] // head
    any_spec = pl.BlockSpec(memory_space=pl.ANY)
    vmem_spec = pl.BlockSpec(memory_space=pltpu.VMEM)
    dma = pltpu.SemaphoreType.DMA
    bf, f32 = jnp.bfloat16, jnp.float32
    new_shape = jax.ShapeDtypeStruct((rows, kv_heads, head), bf)
    return pl.pallas_call(
        functools.partial(front_kernel, ny, nx),
        out_shape=(jax.ShapeDtypeStruct((nx, rows, heads // nx * head), bf), new_shape, new_shape),
        in_specs=[any_spec] * 6 + [pl.BlockSpec(memory_space=pltpu.SMEM)],
        out_specs=(vmem_spec,) * 3,
        scratch_shapes=[
            pltpu.VMEM((batch, width), bf), pltpu.VMEM(w_query.shape, bf), pltpu.VMEM((width, 2 * kv_cols), bf),
            pltpu.VMEM((batch, w_query.shape[1]), f32), pltpu.VMEM((rows, 2 * kv_cols), f32),
            pltpu.VMEM((nm, rows, w_query.shape[1]), bf), pltpu.VMEM((nm, rows, w_query.shape[1]), bf),
            pltpu.VMEM((rows * heads, head), f32),
            pltpu.VMEM((rows, 2 * kv_cols), bf), pltpu.VMEM((ny, rows, 2 * kv_cols), bf), pltpu.VMEM((2 * groups, rows, head), f32),
            pltpu.VMEM((2, rows * kv_heads, head), f32), pltpu.VMEM((rows * heads, head), f32),
            pltpu.VMEM((SLOTS, groups, context, head), bf), pltpu.VMEM((SLOTS, groups, context, head), bf),
            dma((CHUNK_K,)), dma((CHUNK_K,)), dma((CHUNK_K,)), dma((CHUNK_K,)), dma((SLOTS,)), dma((SLOTS,)),
            dma((nm,)), dma((nm,)), dma((ny,)), dma((ny,)),
        ],
        compiler_params=pltpu.CompilerParams(collective_id=5, has_side_effects=True, vmem_limit_bytes=48 * 1024 * 1024),
        name="front",
    )(tokens, w_query, w_key, w_value, key_cache, value_cache, lengths)


def solution(mesh):
    heads_count = mesh.shape["heads"]
    model_count = mesh.shape["model"]

    def local_step(tokens, w_query, w_key, w_value, w_out, key_cache, value_cache, lengths):
        chips = model_count // 2
        o_parts, key_new, value_new = front(heads_count, chips, tokens, w_query, w_key, w_value, key_cache, value_cache, lengths)
        out_tokens = mix(heads_count, chips, o_parts, w_out, tokens).reshape(tokens.shape)
        return (out_tokens, key_new, value_new)

    cache_spec = P(("replica", "model"), None, None, None)
    new_spec = P(("replica", "model"), None, None)
    return jax.shard_map(
        local_step,
        mesh=mesh,
        in_specs=(P("replica", None), P(None, ("heads", "model")), P(None, None), P(None, None), P(("heads", "model"), None), cache_spec, cache_spec, P(("replica", "model"))),
        out_specs=(P("replica", None), new_spec, new_spec),
        check_vma=False,
    )
```

```python
import functools

import jax
import jax.numpy as jnp
from jax import lax
from jax.experimental import pallas as pl
from jax.experimental.pallas import tpu as pltpu
from jax.sharding import PartitionSpec as P

MESH = pl.DeviceIdType.MESH
CHUNKS = 4
CHUNK_K = 8
SLOTS = 16
SEQS = 4


def layer_kernel(ny, nx, tok_ref, wq_ref, wk_ref, wv_ref, wo_ref, kc_ref, vc_ref, len_ref,
                 out_ref, kn_ref, vn_ref,
                 x_buf, wq_buf, wkv_buf, acc_q, acc_kv, q_send, q_recv, q_rows, kv_send, kv_all, kv_rows, kn_rows, o_rows, k_buf, v_buf,
                 w_buf, o_send, o_all, part, recv1, recv2,
                 x_sem, wq_sem, wk_sem, wv_sem, k_sem, v_sem, w_sem, sem_q, sem_kv, sem_o, sems1, sems2, sems3, sems4, sems_d):
    y = lax.axis_index("heads")
    model = lax.axis_index("model")
    x = lax.div(model, 2)
    core = lax.rem(model, 2)
    nm = 2 * nx
    batch, width = x_buf.shape
    rows = batch // nm
    kc = width // CHUNK_K
    head = kc_ref.shape[3]
    context = kc_ref.shape[2]
    groups = kc_ref.shape[1] // ny
    kv_cols = groups * head
    hl = wq_ref.shape[1] // head
    heads = nm * hl
    per_group = heads // groups
    depth = wo_ref.shape[0]
    cols = width // 2
    half = cols // 2
    block = half // 4
    hg = nm // 2
    r = rows // CHUNKS

    def dev(yy, xx, cc):
        return {"heads": lax.rem(yy + ny, ny), "model": 2 * lax.rem(xx + nx, nx) + cc}

    def dev_m(mm):
        return {"heads": y, "model": lax.rem(mm + nm, nm)}

    partner = dev(y, x, 1 - core)
    x_next, x_prev = dev(y, x + 1, core), dev(y, x - 1, core)
    y_next, y_prev = dev(y + 1, x, core), dev(y - 1, x, core)

    barrier = pltpu.get_barrier_semaphore()
    peers = [dev_m(model + s) for s in range(1, nm)] + [dev(y + s, x, core) for s in range(1, ny)]
    for peer in peers:
        pl.semaphore_signal(barrier, inc=1, device_id=peer, device_id_type=MESH)

    sends = []

    def remote(src, dst, send_sem, recv_sem, target):
        copy = pltpu.make_async_remote_copy(src_ref=src, dst_ref=dst, send_sem=send_sem, recv_sem=recv_sem,
                                            device_id=target, device_id_type=MESH)
        copy.start()
        sends.append(copy)

    def arrive(dst, sem):
        pltpu.make_async_copy(dst, dst, sem).wait()

    copies = {}
    kv_here = pl.ds(pl.multiple_of(y * kv_cols, kv_cols), kv_cols)
    for i in range(CHUNK_K):
        ks = pl.ds(i * kc, kc)
        copies["x", i] = pltpu.make_async_copy(tok_ref.at[:, ks], x_buf.at[:, ks], x_sem.at[i])
        copies["q", i] = pltpu.make_async_copy(wq_ref.at[ks], wq_buf.at[ks], wq_sem.at[i])
        copies["x", i].start()
        copies["q", i].start()

    def cache_copies(b, slot):
        gs = pl.ds(y * groups, groups)
        return (pltpu.make_async_copy(kc_ref.at[b, gs], k_buf.at[slot], k_sem.at[slot]),
                pltpu.make_async_copy(vc_ref.at[b, gs], v_buf.at[slot], v_sem.at[slot]))

    for i in range(CHUNK_K):
        ks = pl.ds(i * kc, kc)
        copies["x", i].wait()
        copies["q", i].wait()
        copies["k", i] = pltpu.make_async_copy(wk_ref.at[ks, kv_here], wkv_buf.at[ks, 0:kv_cols], wk_sem.at[i])
        copies["v", i] = pltpu.make_async_copy(wv_ref.at[ks, kv_here], wkv_buf.at[ks, kv_cols:2 * kv_cols], wv_sem.at[i])
        copies["k", i].start()
        copies["v", i].start()
        prod = jnp.dot(x_buf[:, ks], wq_buf[ks, :], preferred_element_type=jnp.float32)
        acc_q[...] = prod if i == 0 else acc_q[...] + prod
    q_send[...] = acc_q[...].astype(jnp.bfloat16).reshape(nm, rows, hl * head)
    pl.semaphore_wait(barrier, len(peers))
    for s in [4, 3, 5, 2, 6, 1, 7]:
        target = lax.rem(model + s, nm)
        remote(q_send.at[target], q_recv.at[model], sem_q.at[0, s], sem_q.at[1, nm - s], dev_m(target))
    q_recv[pl.ds(model, 1)] = q_send[pl.ds(model, 1)]

    mine = pl.ds(pl.multiple_of(model * rows, rows), rows)
    for i in range(CHUNK_K):
        ks = pl.ds(i * kc, kc)
        copies["k", i].wait()
        copies["v", i].wait()
        for b in range(i * SLOTS // CHUNK_K, (i + 1) * SLOTS // CHUNK_K):
            for copy in cache_copies(b, b):
                copy.start()
        prod = jnp.dot(x_buf[mine, ks], wkv_buf[ks, :], preferred_element_type=jnp.float32)
        acc_kv[...] = prod if i == 0 else acc_kv[...] + prod
    kv_bf = acc_kv[...].astype(jnp.bfloat16)
    kv_send[...] = kv_bf
    kv_all[pl.ds(y, 1)] = kv_bf[None]
    for j in range(2 * groups):
        kv_rows[j] = kv_bf[:, j * head:(j + 1) * head].astype(jnp.float32)
    for s in (2, 1, 3):
        remote(kv_send, kv_all.at[y], sem_kv.at[0, s], sem_kv.at[1, ny - s], dev(y + s, x, core))

    my_cols = pl.ds(pl.multiple_of(core * cols, cols), cols)
    other_cols = pl.ds(pl.multiple_of((1 - core) * cols, cols), cols)
    my_rows = pl.ds(pl.multiple_of(core * depth, depth), depth)
    other_rows = pl.ds(pl.multiple_of((1 - core) * depth, depth), depth)
    own_w = pltpu.make_async_copy(wo_ref.at[:, my_cols], w_buf.at[my_rows], w_sem.at[2])
    own_w.start()
    remote(wo_ref.at[:, other_cols], w_buf.at[my_rows], w_sem.at[0], w_sem.at[1], partner)

    for s in range(1, nm):
        arrive(q_recv.at[lax.rem(model + s, nm)], sem_q.at[1, s])
    for src in range(nm):
        for j in range(hl):
            q_rows[pl.ds(src * hl + j, rows, stride=heads), :] = q_recv[src, :, j * head:(j + 1) * head].astype(jnp.float32)

    scale = head ** -0.5
    hc = heads // nx

    def attend(k):
        def step(n, carry):
            positions = lax.broadcasted_iota(jnp.int32, (per_group, context), 1)
            pairs, scores, news = [], [], []
            for u in range(SEQS):
                b = k * r + n * SEQS + u
                slot = lax.rem(b, SLOTS)
                for copy in cache_copies(b, slot):
                    copy.wait()
                length = len_ref[b]
                for g in range(groups):
                    q = q_rows[pl.ds(pl.multiple_of(b * heads + g * per_group, per_group), per_group), :]
                    s = lax.dot_general(q.astype(jnp.bfloat16), k_buf[slot, g], (((1,), (1,)), ((), ())), preferred_element_type=jnp.float32) * scale
                    s = jnp.where(positions < length, s, -jnp.inf)
                    s_new = jnp.sum(q * kv_rows[g, pl.ds(b, 1), :], axis=1, keepdims=True) * scale
                    pairs.append((b, slot, g))
                    scores.append(s)
                    news.append(s_new)
            tops = [jnp.maximum(jnp.max(s, axis=1, keepdims=True), s_new) for s, s_new in zip(scores, news)]
            weights = [jnp.exp(s - m) for s, m in zip(scores, tops)]
            weight_news = [jnp.exp(s_new - m) for s_new, m in zip(news, tops)]
            sums = [jnp.sum(e, axis=1, keepdims=True) + e_new for e, e_new in zip(weights, weight_news)]
            for (b, slot, g), e, e_new, l in zip(pairs, weights, weight_news, sums):
                out = jnp.dot(e.astype(jnp.bfloat16), v_buf[slot, g], preferred_element_type=jnp.float32)
                out = out + e_new.astype(jnp.bfloat16).astype(jnp.float32) * kv_rows[groups + g, pl.ds(b, 1), :]
                o_rows[pl.ds(pl.multiple_of(b * heads + g * per_group, per_group), per_group), :] = out / l
            if (k + 1) * r + SLOTS <= rows:
                for u in range(SEQS):
                    b = k * r + n * SEQS + u
                    for copy in cache_copies(b + SLOTS, lax.rem(b, SLOTS)):
                        copy.start()
            return carry

        lax.fori_loop(0, r // SEQS, step, 0)
        for h in range(heads):
            o_send[k, h // hc, :, (h % hc) * head:(h % hc + 1) * head] = o_rows[pl.ds(k * r * heads + h, r, stride=heads), :].astype(jnp.bfloat16)
        for s in [4, 3, 5, 2, 6, 1, 7]:
            target = lax.rem(model + s, nm)
            remote(o_send.at[k, lax.div(target, 2)], o_all.at[k, model], sem_o.at[k, 0, s], sem_o.at[k, 1, nm - s], dev_m(target))
        o_all[k, pl.ds(model, 1)] = o_send[k, pl.ds(x, 1)]

    pos1 = (x, y)
    pos2 = (y, x)
    nexts = ((x_next, y_next), (y_next, x_next))
    prevs = ((x_prev, y_prev), (y_prev, x_prev))

    def cols_of(h, d):
        return pl.ds(pl.multiple_of(h * half + lax.rem(d + 4, 4) * block, block), block)

    def compute(k, h, d):
        lhs = o_all[k].reshape(nm * r, o_all.shape[3])
        acc = jnp.dot(lhs, w_buf[:, cols_of(h, d)], preferred_element_type=jnp.float32)
        part[:, k * r:(k + 1) * r, cols_of(h, d)] = acc.reshape(nm, r, block)

    low, high = pl.ds(0, hg), pl.ds(hg, hg)

    def send1(k, h, i, mi, d, target):
        kr = pl.ds(k * r, r)
        remote(part.at[mi, kr, cols_of(h, d)], recv1.at[h, i, :, kr, :], sems1.at[k, h, 0, i], sems1.at[k, h, 1, i], target)

    def wait1(k, h, i):
        arrive(recv1.at[h, i, :, pl.ds(k * r, r), :], sems1.at[k, h, 1, i])

    def s0(k):
        for s in range(1, nm):
            arrive(o_all.at[k, lax.rem(model + s, nm)], sem_o.at[k, 1, s])
        if k == 0:
            own_w.wait()
            arrive(w_buf.at[other_rows], w_sem.at[1])
        for h in range(2):
            p = pos1[h]
            compute(k, h, p + 2)
            send1(k, h, 0, low, p + 2, nexts[h][0])
            send1(k, h, 1, high, p + 2, prevs[h][0])
        for h in range(2):
            p = pos1[h]
            compute(k, h, p + 1)
            send1(k, h, 2, high, p + 1, nexts[h][0])
            compute(k, h, p - 1)
            send1(k, h, 3, low, p - 1, prevs[h][0])
        for h in range(2):
            compute(k, h, pos1[h])

    def s1(k):
        ks = slice(k * r, (k + 1) * r)
        for h in range(2):
            p = pos1[h]
            c = cols_of(h, p + 1)
            wait1(k, h, 0)
            part[0:hg, ks, c] = part[0:hg, ks, c] + recv1[h, 0, :, ks, :]
            send1(k, h, 4, low, p + 1, nexts[h][0])
            c = cols_of(h, p - 1)
            wait1(k, h, 1)
            part[hg:nm, ks, c] = part[hg:nm, ks, c] + recv1[h, 1, :, ks, :]
            send1(k, h, 5, high, p - 1, prevs[h][0])

    def send2(h, i, mi, target):
        remote(part.at[mi, :, cols_of(h, pos1[h])], recv2.at[h, i], sems2.at[h, 0, i], sems2.at[h, 1, i], target)

    def wait2(h, i):
        arrive(recv2.at[h, i], sems2.at[h, 1, i])

    def around(q):
        return lax.rem(q + 2, 4), lax.rem(q + 1, 4), lax.rem(q + 3, 4)

    def s2():
        for h in range(2):
            c = cols_of(h, pos1[h])
            far, up, down = around(pos2[h])
            for k in range(CHUNKS):
                for i in (2, 3, 4, 5):
                    wait1(k, h, i)
            part[0:hg, :, c] = part[0:hg, :, c] + recv1[h, 3] + recv1[h, 4]
            part[hg:nm, :, c] = part[hg:nm, :, c] + recv1[h, 2] + recv1[h, 5]
            send2(h, 0, 2 * far, nexts[h][1])
            send2(h, 1, 2 * far + 1, prevs[h][1])
            send2(h, 2, 2 * up + 1, nexts[h][1])
            send2(h, 3, 2 * down, prevs[h][1])

    def s3():
        for h in range(2):
            c = cols_of(h, pos1[h])
            far, up, down = around(pos2[h])
            wait2(h, 0)
            part[2 * up, :, c] = part[2 * up, :, c] + recv2[h, 0]
            send2(h, 4, 2 * up, nexts[h][1])
            wait2(h, 1)
            part[2 * down + 1, :, c] = part[2 * down + 1, :, c] + recv2[h, 1]
            send2(h, 5, 2 * down + 1, prevs[h][1])

    def region(h, j, d, sub=None, cc=None):
        c0 = pl.multiple_of((core if cc is None else cc) * cols + h * half + lax.rem(d + 4, 4) * block, block)
        j = lax.rem(j + 4, 4)
        mi = pl.ds(2 * j, 2) if sub is None else pl.ds(2 * j + sub, 1)
        return out_ref.at[mi, :, pl.ds(c0, block)]

    def push(reg, sems, index, target):
        remote(reg, reg, sems.at[(0,) + index], sems.at[(1,) + index], target)

    def pulled(reg, sems, index):
        arrive(reg, sems.at[(1,) + index])

    def spread(h, n, j):
        p = pos1[h]
        push(region(h, j, p), sems4, (h, n, 0), nexts[h][0])
        push(region(h, j, p), sems4, (h, n, 1), prevs[h][0])
        push(region(h, j, p), sems_d, (h, n, 0), partner)

    def relay(h, n, j):
        p = pos1[h]
        pulled(region(h, j, p - 1), sems4, (h, n, 0))
        push(region(h, j, p - 1, 0), sems4, (h, n, 2), nexts[h][0])
        push(region(h, j, p - 1), sems_d, (h, n, 1), partner)
        pulled(region(h, j, p + 1), sems4, (h, n, 1))
        push(region(h, j, p + 1, 1), sems4, (h, n, 3), prevs[h][0])
        push(region(h, j, p + 1), sems_d, (h, n, 2), partner)

    def finish(h, n, j):
        p = pos1[h]
        for sub in range(2):
            reg = region(h, j, p + 2, sub)
            pulled(reg, sems4, (h, n, 2 + sub))
            push(reg, sems_d, (h, n, 3 + sub), partner)

    def s4():
        for h in range(2):
            p, q = pos1[h], pos2[h]
            c = cols_of(h, p)
            for i in (2, 3, 4, 5):
                wait2(h, i)
            oc = pl.ds(pl.multiple_of(core * cols + h * half + p * block, block), block)
            for sub, plain, summed in ((0, 3, 4), (1, 2, 5)):
                mi = 2 * q + sub
                total = part[mi, :, c] + recv2[h, plain] + recv2[h, summed]
                total = x_buf[pl.ds(pl.multiple_of(mi * rows, rows), rows), oc].astype(jnp.float32) + total
                out_ref[mi, :, oc] = total.astype(out_ref.dtype)
            push(region(h, q, p), sems3, (h, 0), nexts[h][1])
            push(region(h, q, p), sems3, (h, 1), prevs[h][1])
        for h in range(2):
            spread(h, 0, pos2[h])

    def s5():
        for h in range(2):
            p, q = pos1[h], pos2[h]
            pulled(region(h, q - 1, p), sems3, (h, 0))
            push(region(h, q - 1, p, 0), sems3, (h, 2), nexts[h][1])
            pulled(region(h, q + 1, p), sems3, (h, 1))
            push(region(h, q + 1, p, 1), sems3, (h, 3), prevs[h][1])
        for h in range(2):
            spread(h, 1, pos2[h] - 1)
            spread(h, 2, pos2[h] + 1)

    def s6():
        for h in range(2):
            relay(h, 0, pos2[h])
        for h in range(2):
            p, q = pos1[h], pos2[h]
            pulled(region(h, q + 2, p, 0), sems3, (h, 2))
            pulled(region(h, q + 2, p, 1), sems3, (h, 3))
            spread(h, 3, q + 2)

    def s7():
        for h in range(2):
            relay(h, 1, pos2[h] - 1)
            relay(h, 2, pos2[h] + 1)
        for h in range(2):
            finish(h, 0, pos2[h])
        for h in range(2):
            relay(h, 3, pos2[h] + 2)
        for n, d in ((1, -1), (2, 1), (3, 2)):
            for h in range(2):
                finish(h, n, pos2[h] + d)

    def new_rows():
        for s in range(1, ny):
            arrive(kv_all.at[lax.rem(y + s, ny)], sem_kv.at[1, s])
        kv_heads = ny * groups
        for half_, ref in ((0, kn_ref), (1, vn_ref)):
            for g in range(kv_heads):
                c0 = half_ * kv_cols + (g % groups) * head
                kn_rows[half_, pl.ds(g, rows, stride=kv_heads), :] = kv_all[g // groups, :, c0:c0 + head].astype(jnp.float32)
            ref[...] = kn_rows[half_].reshape(rows, kv_heads, head).astype(jnp.bfloat16)

    attend(0)
    attend(1)
    s0(0)
    attend(2)
    s1(0)
    s0(1)
    attend(3)
    s1(1)
    s0(2)
    new_rows()
    s1(2)
    s0(3)
    s1(3)
    s2()
    s3()
    s4()
    s5()
    s6()
    s7()
    for h in range(2):
        p, q = pos1[h], pos2[h]
        for n, d in ((0, 0), (1, -1), (2, 1), (3, 2)):
            for i, (dp, sub) in enumerate(((0, None), (-1, None), (1, None), (2, 0), (2, 1))):
                pulled(region(h, q + d, p + dp, sub, 1 - core), sems_d, (h, n, i))
    for copy in sends:
        copy.wait_send()


def layer(ny, nx, tokens, w_query, w_key, w_value, w_out, key_cache, value_cache, lengths):
    batch, width = tokens.shape
    rows, kv_heads, context, head = key_cache.shape
    nm = 2 * nx
    groups = kv_heads // ny
    kv_cols = groups * head
    heads = nm * w_query.shape[1] // head
    depth = w_out.shape[0]
    block = width // 16
    r = rows // CHUNKS
    hbm_spec = pl.BlockSpec(memory_space=pltpu.HBM)
    vmem_spec = pl.BlockSpec(memory_space=pltpu.VMEM)
    dma = pltpu.SemaphoreType.DMA
    bf, f32 = jnp.bfloat16, jnp.float32
    new_shape = jax.ShapeDtypeStruct((rows, kv_heads, head), bf)
    return pl.pallas_call(
        functools.partial(layer_kernel, ny, nx),
        out_shape=(jax.ShapeDtypeStruct((nm, rows, width), bf), new_shape, new_shape),
        in_specs=[hbm_spec] * 7 + [pl.BlockSpec(memory_space=pltpu.SMEM)],
        out_specs=(vmem_spec,) * 3,
        scratch_shapes=[
            pltpu.VMEM((batch, width), bf), pltpu.VMEM(w_query.shape, bf), pltpu.VMEM((width, 2 * kv_cols), bf),
            pltpu.VMEM((batch, w_query.shape[1]), f32), pltpu.VMEM((rows, 2 * kv_cols), f32),
            pltpu.VMEM((nm, rows, w_query.shape[1]), bf), pltpu.VMEM((nm, rows, w_query.shape[1]), bf),
            pltpu.VMEM((rows * heads, head), f32),
            pltpu.VMEM((rows, 2 * kv_cols), bf), pltpu.VMEM((ny, rows, 2 * kv_cols), bf), pltpu.VMEM((2 * groups, rows, head), f32),
            pltpu.VMEM((2, rows * kv_heads, head), f32), pltpu.VMEM((rows * heads, head), f32),
            pltpu.VMEM((SLOTS, groups, context, head), bf), pltpu.VMEM((SLOTS, groups, context, head), bf),
            pltpu.VMEM((2 * depth, width // 2), bf),
            pltpu.VMEM((CHUNKS, nx, r, 2 * depth), bf), pltpu.VMEM((CHUNKS, nm, r, 2 * depth), bf),
            pltpu.VMEM((nm, rows, width // 2), f32),
            pltpu.VMEM((2, 6, nm // 2, rows, block), f32),
            pltpu.VMEM((2, 6, rows, block), f32),
            dma((CHUNK_K,)), dma((CHUNK_K,)), dma((CHUNK_K,)), dma((CHUNK_K,)), dma((SLOTS,)), dma((SLOTS,)), dma((3,)),
            dma((2, nm)), dma((2, ny)), dma((CHUNKS, 2, nm)), dma((CHUNKS, 2, 2, 6)), dma((2, 2, 6)), dma((2, 2, 4)),
            dma((2, 2, 4, 4)), dma((2, 2, 4, 5)),
        ],
        compiler_params=pltpu.CompilerParams(collective_id=5, has_side_effects=True, vmem_limit_bytes=47 * 1024 * 1024),
        name="layer",
    )(tokens, w_query, w_key, w_value, w_out, key_cache, value_cache, lengths)


def solution(mesh):
    heads_count = mesh.shape["heads"]
    chips = mesh.shape["model"] // 2

    def local_step(tokens, w_query, w_key, w_value, w_out, key_cache, value_cache, lengths):
        out, key_new, value_new = layer(heads_count, chips, tokens, w_query, w_key, w_value, w_out, key_cache, value_cache, lengths)
        return (out.reshape(tokens.shape), key_new, value_new)

    cache_spec = P(("replica", "model"), None, None, None)
    new_spec = P(("replica", "model"), None, None)
    return jax.shard_map(
        local_step,
        mesh=mesh,
        in_specs=(P("replica", None), P(None, ("heads", "model")), P(None, None), P(None, None), P(("heads", "model"), None), cache_spec, cache_spec, P(("replica", "model"))),
        out_specs=(P("replica", None), new_spec, new_spec),
        check_vma=False,
    )
```

```python
import functools

import jax
import jax.numpy as jnp
from jax import lax
from jax.experimental import pallas as pl
from jax.experimental.pallas import tpu as pltpu
from jax.sharding import PartitionSpec as P

MESH = pl.DeviceIdType.MESH
CHUNKS = 4
CHUNK_K = 8
SLOTS = 16
SEQS = 4
AHEAD = 6


def layer_kernel(ny, nx, tok_ref, wq_ref, wk_ref, wv_ref, wo_ref, kc_ref, vc_ref, len_ref,
                 out_ref, kn_ref, vn_ref,
                 x_buf, wq_buf, wkv_buf, acc_q, acc_kv, q_send, q_recv, q_rows, kv_send, kv_all, kv_rows, kn_rows, o_rows, k_buf, v_buf,
                 w_all, w_pass, o_row, o_col, part, recv2,
                 x_sem, wq_sem, wk_sem, wv_sem, k_sem, v_sem, own_sem, sem_pair, sem_w, sem_r, sem_q, sem_kv, sem_row, sem_col, sem_pass,
                 sems2, sems3, sems4, sems_d):
    y = lax.axis_index("heads")
    model = lax.axis_index("model")
    x = lax.div(model, 2)
    core = lax.rem(model, 2)
    nm = 2 * nx
    batch, width = x_buf.shape
    rows = batch // nm
    kc = width // CHUNK_K
    head = kc_ref.shape[3]
    context = kc_ref.shape[2]
    groups = kc_ref.shape[1] // ny
    kv_cols = groups * head
    hl = wq_ref.shape[1] // head
    heads = nm * hl
    per_group = heads // groups
    depth = wo_ref.shape[0]
    cols = width // 2
    half = cols // 2
    block = half // 4
    near = depth // 2
    r = rows // CHUNKS

    def dev(yy, xx, cc):
        return {"heads": lax.rem(yy + ny, ny), "model": 2 * lax.rem(xx + nx, nx) + cc}

    def dev_m(mm):
        return {"heads": y, "model": lax.rem(mm + nm, nm)}

    partner = dev(y, x, 1 - core)
    x_next, x_prev = dev(y, x + 1, core), dev(y, x - 1, core)
    y_next, y_prev = dev(y + 1, x, core), dev(y - 1, x, core)

    barrier = pltpu.get_barrier_semaphore()
    peers = [dev_m(model + s) for s in range(1, nm)] + [dev(y + s, x, core) for s in range(1, ny)]
    peers += [dev(y + 1, x, 1 - core), dev(y - 1, x, 1 - core)]
    for peer in peers:
        pl.semaphore_signal(barrier, inc=1, device_id=peer, device_id_type=MESH)

    sends = []

    def remote(src, dst, send_sem, recv_sem, target):
        copy = pltpu.make_async_remote_copy(src_ref=src, dst_ref=dst, send_sem=send_sem, recv_sem=recv_sem,
                                            device_id=target, device_id_type=MESH)
        copy.start()
        sends.append(copy)

    def arrive(dst, sem):
        pltpu.make_async_copy(dst, dst, sem).wait()

    pos1 = (x, y)
    pos2 = (y, x)
    nexts = ((x_next, y_next), (y_next, x_next))
    prevs = ((x_prev, y_prev), (y_prev, x_prev))
    halves = (pl.ds(0, near), pl.ds(near, near))

    def along(h, d, cc):
        return dev(y, x + d, cc) if h == 0 else dev(y + d, x, cc)

    def block_of(h, d, cc):
        return pl.ds(pl.multiple_of(cc * cols + h * half + lax.rem(d + 4, 4) * block, block), block)

    def slot_of(h, d, cc):
        return 2 * lax.rem(pos1[h] + d + 4, 4) + cc

    def far_start(cc):
        for h in range(2):
            for way, target in ((0, nexts[h][0]), (1, prevs[h][0])):
                remote(wo_ref.at[halves[way], block_of(h, pos1[h] + 2, cc)], w_pass.at[h, way, cc],
                       sem_r.at[0, h, way, cc], sem_r.at[1, h, way, cc], target)

    def near_start(cc, n):
        for h in range(2):
            for way, d in ((0, 1), (1, -1)):
                remote(wo_ref.at[halves[n], block_of(h, pos1[h] + d, cc)], w_all.at[h, slot_of(h, 0, core), halves[n]],
                       sem_w.at[0, h, way, cc, n], sem_w.at[1, h, way, core, n], along(h, d, cc))

    def far_pass(cc):
        for h in range(2):
            for way, d in ((0, 1), (1, -1)):
                arrive(w_pass.at[h, way, cc], sem_r.at[1, h, way, cc])
                remote(w_pass.at[h, way, cc], w_all.at[h, slot_of(h, -d, core), halves[way]],
                       sem_w.at[0, h, way, cc, 2], sem_w.at[1, h, way, core, 2], along(h, d, cc))

    own_copies = []

    def own_start():
        for h in range(2):
            copy = pltpu.make_async_copy(wo_ref.at[:, block_of(h, pos1[h], core)], w_all.at[h, slot_of(h, 0, core)], own_sem.at[h])
            copy.start()
            own_copies.append(copy)
            remote(wo_ref.at[:, block_of(h, pos1[h], 1 - core)], w_all.at[h, slot_of(h, 0, core)], sem_pair.at[0, h], sem_pair.at[1, h], partner)

    def weights_here():
        for h in range(2):
            own_copies[h].wait()
            arrive(w_all.at[h, slot_of(h, 0, 1 - core)], sem_pair.at[1, h])
            for way, d in ((0, -1), (1, 1)):
                for cc in range(2):
                    for n in range(2):
                        arrive(w_all.at[h, slot_of(h, d, cc), halves[n]], sem_w.at[1, h, way, cc, n])
                    arrive(w_all.at[h, slot_of(h, 2, cc), halves[way]], sem_w.at[1, h, way, cc, 2])

    copies = {}
    kv_here = pl.ds(pl.multiple_of(y * kv_cols, kv_cols), kv_cols)
    for i in range(CHUNK_K):
        ks = pl.ds(i * kc, kc)
        copies["x", i] = pltpu.make_async_copy(tok_ref.at[:, ks], x_buf.at[:, ks], x_sem.at[i])
        copies["q", i] = pltpu.make_async_copy(wq_ref.at[ks], wq_buf.at[ks], wq_sem.at[i])
        copies["k", i] = pltpu.make_async_copy(wk_ref.at[ks, kv_here], wkv_buf.at[ks, 0:kv_cols], wk_sem.at[i])
        copies["v", i] = pltpu.make_async_copy(wv_ref.at[ks, kv_here], wkv_buf.at[ks, kv_cols:2 * kv_cols], wv_sem.at[i])

    def cache_copies(b, slot):
        gs = pl.ds(y * groups, groups)
        return (pltpu.make_async_copy(kc_ref.at[b, gs], k_buf.at[slot], k_sem.at[slot]),
                pltpu.make_async_copy(vc_ref.at[b, gs], v_buf.at[slot], v_sem.at[slot]))

    reads = [(copies["x", i], copies["q", i]) for i in range(CHUNK_K)] + [(copies["k", i], copies["v", i]) for i in range(CHUNK_K)]
    reads += [cache_copies(b, b) for b in range(SLOTS)]

    def read_next(n):
        for pair in reads[:n]:
            for copy in pair:
                copy.start()
        del reads[:n]

    read_next(AHEAD)
    pl.semaphore_wait(barrier, len(peers))
    far_start(0)
    for i in range(CHUNK_K):
        ks = pl.ds(i * kc, kc)
        copies["x", i].wait()
        copies["q", i].wait()
        read_next(1)
        prod = jnp.dot(x_buf[:, ks], wq_buf[ks, :], preferred_element_type=jnp.float32)
        acc_q[...] = prod if i == 0 else acc_q[...] + prod
    q_send[...] = acc_q[...].astype(jnp.bfloat16).reshape(nm, rows, hl * head)
    for s in [4, 3, 5, 2, 6, 1, 7]:
        target = lax.rem(model + s, nm)
        remote(q_send.at[target], q_recv.at[model], sem_q.at[0, s], sem_q.at[1, nm - s], dev_m(target))
    q_recv[pl.ds(model, 1)] = q_send[pl.ds(model, 1)]
    far_start(1)
    near_start(0, 0)

    mine = pl.ds(pl.multiple_of(model * rows, rows), rows)
    for i in range(CHUNK_K):
        ks = pl.ds(i * kc, kc)
        copies["k", i].wait()
        copies["v", i].wait()
        read_next(1)
        prod = jnp.dot(x_buf[mine, ks], wkv_buf[ks, :], preferred_element_type=jnp.float32)
        acc_kv[...] = prod if i == 0 else acc_kv[...] + prod
    kv_bf = acc_kv[...].astype(jnp.bfloat16)
    kv_send[...] = kv_bf
    kv_all[pl.ds(y, 1)] = kv_bf[None]
    for j in range(2 * groups):
        kv_rows[j] = kv_bf[:, j * head:(j + 1) * head].astype(jnp.float32)
    for s in (2, 1, 3):
        remote(kv_send, kv_all.at[y], sem_kv.at[0, s], sem_kv.at[1, ny - s], dev(y + s, x, core))

    near_start(0, 1)
    own_start()
    read_next(len(reads))
    for s in range(1, nm):
        arrive(q_recv.at[lax.rem(model + s, nm)], sem_q.at[1, s])
    for src in range(nm):
        for j in range(hl):
            q_rows[pl.ds(src * hl + j, rows, stride=heads), :] = q_recv[src, :, j * head:(j + 1) * head].astype(jnp.float32)

    scale = head ** -0.5
    hc = heads // nx

    def attend(k):
        def step(n, carry):
            positions = lax.broadcasted_iota(jnp.int32, (per_group, context), 1)
            pairs, scores, news = [], [], []
            for u in range(SEQS):
                b = k * r + n * SEQS + u
                slot = lax.rem(b, SLOTS)
                for copy in cache_copies(b, slot):
                    copy.wait()
                length = len_ref[b]
                for g in range(groups):
                    q = q_rows[pl.ds(pl.multiple_of(b * heads + g * per_group, per_group), per_group), :]
                    s = lax.dot_general(q.astype(jnp.bfloat16), k_buf[slot, g], (((1,), (1,)), ((), ())), preferred_element_type=jnp.float32) * scale
                    s = jnp.where(positions < length, s, -jnp.inf)
                    s_new = jnp.sum(q * kv_rows[g, pl.ds(b, 1), :], axis=1, keepdims=True) * scale
                    pairs.append((b, slot, g))
                    scores.append(s)
                    news.append(s_new)
            tops = [jnp.maximum(jnp.max(s, axis=1, keepdims=True), s_new) for s, s_new in zip(scores, news)]
            weights = [jnp.exp(s - m) for s, m in zip(scores, tops)]
            weight_news = [jnp.exp(s_new - m) for s_new, m in zip(news, tops)]
            sums = [jnp.sum(e, axis=1, keepdims=True) + e_new for e, e_new in zip(weights, weight_news)]
            for (b, slot, g), e, e_new, l in zip(pairs, weights, weight_news, sums):
                out = jnp.dot(e.astype(jnp.bfloat16), v_buf[slot, g], preferred_element_type=jnp.float32)
                out = out + e_new.astype(jnp.bfloat16).astype(jnp.float32) * kv_rows[groups + g, pl.ds(b, 1), :]
                o_rows[pl.ds(pl.multiple_of(b * heads + g * per_group, per_group), per_group), :] = out / l
            if (k + 1) * r + SLOTS <= rows:
                for u in range(SEQS):
                    b = k * r + n * SEQS + u
                    for copy in cache_copies(b + SLOTS, lax.rem(b, SLOTS)):
                        copy.start()
            return carry

        lax.fori_loop(0, r // SEQS, step, 0)
        for h in range(heads):
            o_row[k, core, x, h // hc, :, (h % hc) * head:(h % hc + 1) * head] = o_rows[pl.ds(k * r * heads + h, r, stride=heads), :].astype(jnp.bfloat16)
        own = o_row.at[k, core, x]
        for d in (2, 1, 3):
            remote(own, own, sem_row.at[0, k, d], sem_row.at[1, k, nx - d], dev(y, x + d, core))
        remote(own, own, sem_pass.at[0, k, 0], sem_pass.at[1, k, 0], partner)

    def columns(k):
        for d in range(1, nx):
            got = o_row.at[k, core, lax.rem(x + d, nx)]
            arrive(got, sem_row.at[1, k, d])
            remote(got, got, sem_pass.at[0, k, d], sem_pass.at[1, k, d], partner)
        for d in (2, 1, 3):
            remote(o_row.at[k, core, :, x], o_col.at[k, y, core], sem_col.at[0, k, d], sem_col.at[1, k, ny - d], dev(y + d, x, core))

    def across(k):
        for d in range(1, ny):
            got = o_col.at[k, lax.rem(y + d, ny), core]
            arrive(got, sem_col.at[1, k, d])
            remote(got, got, sem_pass.at[0, k, 3 + d], sem_pass.at[1, k, 3 + d], partner)

    def project(k):
        for d in range(nx):
            arrive(o_row.at[k, 1 - core, lax.rem(x + d, nx)], sem_pass.at[1, k, d])
        for d in range(1, ny):
            arrive(o_col.at[k, lax.rem(y + d, ny), 1 - core], sem_pass.at[1, k, 3 + d])
        ks = slice(k * r, (k + 1) * r)
        hw = o_row.shape[5]
        acc = jnp.zeros((nm * r, block), jnp.float32)
        for b in range(nx):
            lhs = o_row[k, :, :, b].reshape(nm * r, hw)
            acc = acc + jnp.dot(lhs, w_all[0, 2 * b:2 * b + 2].reshape(hw, block), preferred_element_type=jnp.float32)
        part[0, :, :, ks, :] = acc.reshape(2, nx, r, block)
        acc = jnp.zeros((nm * r, block), jnp.float32)
        for d in range(ny):
            yy = lax.rem(y + d, ny)
            lhs = o_row[k, :, :, x] if d == 0 else o_col[k, yy]
            acc = acc + jnp.dot(lhs.reshape(nm * r, hw), w_all[1, pl.ds(2 * yy, 2)].reshape(hw, block), preferred_element_type=jnp.float32)
        part[1, :, :, ks, :] = acc.reshape(2, nx, r, block)

    def send2(h, i, sub, q, target):
        remote(part.at[h, sub, q], recv2.at[h, i], sems2.at[0, h, i], sems2.at[1, h, i], target)

    def wait2(h, i):
        arrive(recv2.at[h, i], sems2.at[1, h, i])

    def around(q):
        return lax.rem(q + 2, 4), lax.rem(q + 1, 4), lax.rem(q + 3, 4)

    def s2():
        for h in range(2):
            far, up, down = around(pos2[h])
            send2(h, 0, 0, far, nexts[h][1])
            send2(h, 1, 1, far, prevs[h][1])
        for h in range(2):
            far, up, down = around(pos2[h])
            send2(h, 2, 1, up, nexts[h][1])
            send2(h, 3, 0, down, prevs[h][1])

    def s3():
        for h in range(2):
            far, up, down = around(pos2[h])
            wait2(h, 0)
            part[h, 0, up] = part[h, 0, up] + recv2[h, 0]
            send2(h, 4, 0, up, nexts[h][1])
            wait2(h, 1)
            part[h, 1, down] = part[h, 1, down] + recv2[h, 1]
            send2(h, 5, 1, down, prevs[h][1])

    def region(h, j, d, sub=None, cc=None):
        c0 = pl.multiple_of((core if cc is None else cc) * cols + h * half + lax.rem(d + 4, 4) * block, block)
        j = lax.rem(j + 4, 4)
        mi = pl.ds(2 * j, 2) if sub is None else pl.ds(2 * j + sub, 1)
        return out_ref.at[mi, :, pl.ds(c0, block)]

    def push(reg, sems, index, target):
        remote(reg, reg, sems.at[(0,) + index], sems.at[(1,) + index], target)

    def pulled(reg, sems, index):
        arrive(reg, sems.at[(1,) + index])

    def spread(h, n, j):
        p = pos1[h]
        push(region(h, j, p), sems4, (h, n, 0), nexts[h][0])
        push(region(h, j, p), sems4, (h, n, 1), prevs[h][0])
        push(region(h, j, p), sems_d, (h, n, 0), partner)

    def relay(h, n, j):
        p = pos1[h]
        pulled(region(h, j, p - 1), sems4, (h, n, 0))
        push(region(h, j, p - 1, 0), sems4, (h, n, 2), nexts[h][0])
        push(region(h, j, p - 1), sems_d, (h, n, 1), partner)
        pulled(region(h, j, p + 1), sems4, (h, n, 1))
        push(region(h, j, p + 1, 1), sems4, (h, n, 3), prevs[h][0])
        push(region(h, j, p + 1), sems_d, (h, n, 2), partner)

    def finish(h, n, j):
        p = pos1[h]
        for sub in range(2):
            reg = region(h, j, p + 2, sub)
            pulled(reg, sems4, (h, n, 2 + sub))
            push(reg, sems_d, (h, n, 3 + sub), partner)

    def s4():
        for h in range(2):
            p, q = pos1[h], pos2[h]
            for i in (2, 3, 4, 5):
                wait2(h, i)
            oc = pl.ds(pl.multiple_of(core * cols + h * half + p * block, block), block)
            for sub, plain, summed in ((0, 3, 4), (1, 2, 5)):
                mi = 2 * q + sub
                total = part[h, sub, q] + recv2[h, plain] + recv2[h, summed]
                total = x_buf[pl.ds(pl.multiple_of(mi * rows, rows), rows), oc].astype(jnp.float32) + total
                out_ref[mi, :, oc] = total.astype(out_ref.dtype)
            push(region(h, q, p), sems3, (h, 0), nexts[h][1])
            push(region(h, q, p), sems3, (h, 1), prevs[h][1])
        for h in range(2):
            spread(h, 0, pos2[h])

    def s5():
        for h in range(2):
            p, q = pos1[h], pos2[h]
            pulled(region(h, q - 1, p), sems3, (h, 0))
            push(region(h, q - 1, p, 0), sems3, (h, 2), nexts[h][1])
            pulled(region(h, q + 1, p), sems3, (h, 1))
            push(region(h, q + 1, p, 1), sems3, (h, 3), prevs[h][1])
        for h in range(2):
            spread(h, 1, pos2[h] - 1)
            spread(h, 2, pos2[h] + 1)

    def s6():
        for h in range(2):
            relay(h, 0, pos2[h])
        for h in range(2):
            p, q = pos1[h], pos2[h]
            pulled(region(h, q + 2, p, 0), sems3, (h, 2))
            pulled(region(h, q + 2, p, 1), sems3, (h, 3))
            spread(h, 3, q + 2)

    def s7():
        for h in range(2):
            relay(h, 1, pos2[h] - 1)
            relay(h, 2, pos2[h] + 1)
        for h in range(2):
            finish(h, 0, pos2[h])
        for h in range(2):
            relay(h, 3, pos2[h] + 2)
        for n, d in ((1, -1), (2, 1), (3, 2)):
            for h in range(2):
                finish(h, n, pos2[h] + d)

    def new_rows():
        for s in range(1, ny):
            arrive(kv_all.at[lax.rem(y + s, ny)], sem_kv.at[1, s])
        kv_heads = ny * groups
        for half_, ref in ((0, kn_ref), (1, vn_ref)):
            for g in range(kv_heads):
                c0 = half_ * kv_cols + (g % groups) * head
                kn_rows[half_, pl.ds(g, rows, stride=kv_heads), :] = kv_all[g // groups, :, c0:c0 + head].astype(jnp.float32)
            ref[...] = kn_rows[half_].reshape(rows, kv_heads, head).astype(jnp.bfloat16)

    near_start(1, 0)
    attend(0)
    far_pass(0)
    attend(1)
    columns(0)
    far_pass(1)
    near_start(1, 1)
    attend(2)
    across(0)
    columns(1)
    new_rows()
    attend(3)
    across(1)
    columns(2)
    columns(3)
    weights_here()
    project(0)
    project(1)
    across(2)
    across(3)
    project(2)
    project(3)
    s2()
    s3()
    s4()
    s5()
    s6()
    s7()
    for h in range(2):
        p, q = pos1[h], pos2[h]
        for n, d in ((0, 0), (1, -1), (2, 1), (3, 2)):
            for i, (dp, sub) in enumerate(((0, None), (-1, None), (1, None), (2, 0), (2, 1))):
                pulled(region(h, q + d, p + dp, sub, 1 - core), sems_d, (h, n, i))
    for copy in sends:
        copy.wait_send()


def layer(ny, nx, tokens, w_query, w_key, w_value, w_out, key_cache, value_cache, lengths):
    batch, width = tokens.shape
    rows, kv_heads, context, head = key_cache.shape
    nm = 2 * nx
    groups = kv_heads // ny
    kv_cols = groups * head
    heads = nm * w_query.shape[1] // head
    depth = w_out.shape[0]
    block = width // 16
    r = rows // CHUNKS
    hbm_spec = pl.BlockSpec(memory_space=pltpu.HBM)
    vmem_spec = pl.BlockSpec(memory_space=pltpu.VMEM)
    dma = pltpu.SemaphoreType.DMA
    bf, f32 = jnp.bfloat16, jnp.float32
    new_shape = jax.ShapeDtypeStruct((rows, kv_heads, head), bf)
    return pl.pallas_call(
        functools.partial(layer_kernel, ny, nx),
        out_shape=(jax.ShapeDtypeStruct((nm, rows, width), bf), new_shape, new_shape),
        in_specs=[hbm_spec] * 7 + [pl.BlockSpec(memory_space=pltpu.SMEM)],
        out_specs=(vmem_spec,) * 3,
        scratch_shapes=[
            pltpu.VMEM((batch, width), bf), pltpu.VMEM(w_query.shape, bf), pltpu.VMEM((width, 2 * kv_cols), bf),
            pltpu.VMEM((batch, w_query.shape[1]), f32), pltpu.VMEM((rows, 2 * kv_cols), f32),
            pltpu.VMEM((nm, rows, w_query.shape[1]), bf), pltpu.VMEM((nm, rows, w_query.shape[1]), bf),
            pltpu.VMEM((rows * heads, head), f32),
            pltpu.VMEM((rows, 2 * kv_cols), bf), pltpu.VMEM((ny, rows, 2 * kv_cols), bf), pltpu.VMEM((2 * groups, rows, head), f32),
            pltpu.VMEM((2, rows * kv_heads, head), f32), pltpu.VMEM((rows * heads, head), f32),
            pltpu.VMEM((SLOTS, groups, context, head), bf), pltpu.VMEM((SLOTS, groups, context, head), bf),
            pltpu.VMEM((2, nm, depth, block), bf), pltpu.VMEM((2, 2, 2, depth // 2, block), bf),
            pltpu.VMEM((CHUNKS, 2, nx, nx, r, 2 * depth), bf), pltpu.VMEM((CHUNKS, ny, 2, nx, r, 2 * depth), bf),
            pltpu.VMEM((2, 2, nx, rows, block), f32),
            pltpu.VMEM((2, 6, rows, block), f32),
            dma((CHUNK_K,)), dma((CHUNK_K,)), dma((CHUNK_K,)), dma((CHUNK_K,)), dma((SLOTS,)), dma((SLOTS,)),
            dma((2,)), dma((2, 2)), dma((2, 2, 2, 2, 3)), dma((2, 2, 2, 2)), dma((2, nm)), dma((2, ny)),
            dma((2, CHUNKS, nx)), dma((2, CHUNKS, ny)), dma((2, CHUNKS, 7)), dma((2, 2, 6)), dma((2, 2, 4)),
            dma((2, 2, 4, 4)), dma((2, 2, 4, 5)),
        ],
        compiler_params=pltpu.CompilerParams(collective_id=5, has_side_effects=True, vmem_limit_bytes=47 * 1024 * 1024),
        name="layer",
    )(tokens, w_query, w_key, w_value, w_out, key_cache, value_cache, lengths)


def solution(mesh):
    heads_count = mesh.shape["heads"]
    chips = mesh.shape["model"] // 2

    def local_step(tokens, w_query, w_key, w_value, w_out, key_cache, value_cache, lengths):
        out, key_new, value_new = layer(heads_count, chips, tokens, w_query, w_key, w_value, w_out, key_cache, value_cache, lengths)
        return (out.reshape(tokens.shape), key_new, value_new)

    cache_spec = P(("replica", "model"), None, None, None)
    new_spec = P(("replica", "model"), None, None)
    return jax.shard_map(
        local_step,
        mesh=mesh,
        in_specs=(P("replica", None), P(None, ("heads", "model")), P(None, None), P(None, None), P(("heads", "model"), None), cache_spec, cache_spec, P(("replica", "model"))),
        out_specs=(P("replica", None), new_spec, new_spec),
        check_vma=False,
    )
```

```python
import functools

import jax
import jax.numpy as jnp
from jax import lax
from jax.experimental import pallas as pl
from jax.experimental.pallas import tpu as pltpu
from jax.sharding import PartitionSpec as P

MESH = pl.DeviceIdType.MESH
CHUNKS = 4
CHUNK_K = 8
SLOTS = 16
SEQS = 4
AHEAD = 4


def layer_kernel(ny, nx, tok_ref, wq_ref, wk_ref, wv_ref, wo_ref, kc_ref, vc_ref, len_ref,
                 out_ref, kn_ref, vn_ref,
                 x_buf, wq_buf, wkv_buf, acc_q, acc_kv, q_send, q_recv, q_rows, kv_send, kv_all, kv_rows, kn_rows, o_rows, k_buf, v_buf,
                 w_buf, o_send, o_all, part, recv1, recv2,
                 x_sem, wq_sem, wk_sem, wv_sem, k_sem, v_sem, w_sem, sem_q, sem_kv, sem_o, sems1, sems2, sems3, sems4, sems_d):
    y = lax.axis_index("heads")
    model = lax.axis_index("model")
    x = lax.div(model, 2)
    core = lax.rem(model, 2)
    nm = 2 * nx
    batch, width = x_buf.shape
    rows = batch // nm
    kc = width // CHUNK_K
    head = kc_ref.shape[3]
    context = kc_ref.shape[2]
    groups = kc_ref.shape[1] // ny
    kv_cols = groups * head
    hl = wq_ref.shape[1] // head
    heads = nm * hl
    per_group = heads // groups
    depth = wo_ref.shape[0]
    cols = width // 2
    half = cols // 2
    block = half // 4
    hg = nm // 2
    r = rows // CHUNKS

    def dev(yy, xx, cc):
        return {"heads": lax.rem(yy + ny, ny), "model": 2 * lax.rem(xx + nx, nx) + cc}

    def dev_m(mm):
        return {"heads": y, "model": lax.rem(mm + nm, nm)}

    partner = dev(y, x, 1 - core)
    x_next, x_prev = dev(y, x + 1, core), dev(y, x - 1, core)
    y_next, y_prev = dev(y + 1, x, core), dev(y - 1, x, core)

    barrier = pltpu.get_barrier_semaphore()
    peers = [dev_m(model + s) for s in range(1, nm)] + [dev(y + s, x, core) for s in range(1, ny)]
    for peer in peers:
        pl.semaphore_signal(barrier, inc=1, device_id=peer, device_id_type=MESH)

    sends = []

    def remote(src, dst, send_sem, recv_sem, target):
        copy = pltpu.make_async_remote_copy(src_ref=src, dst_ref=dst, send_sem=send_sem, recv_sem=recv_sem,
                                            device_id=target, device_id_type=MESH)
        copy.start()
        sends.append(copy)

    def arrive(dst, sem):
        pltpu.make_async_copy(dst, dst, sem).wait()

    copies = {}
    kv_here = pl.ds(pl.multiple_of(y * kv_cols, kv_cols), kv_cols)
    for i in range(CHUNK_K):
        ks = pl.ds(i * kc, kc)
        copies["x", i] = pltpu.make_async_copy(tok_ref.at[:, ks], x_buf.at[:, ks], x_sem.at[i])
        copies["q", i] = pltpu.make_async_copy(wq_ref.at[ks], wq_buf.at[ks], wq_sem.at[i])
        copies["k", i] = pltpu.make_async_copy(wk_ref.at[ks, kv_here], wkv_buf.at[ks, 0:kv_cols], wk_sem.at[i])
        copies["v", i] = pltpu.make_async_copy(wv_ref.at[ks, kv_here], wkv_buf.at[ks, kv_cols:2 * kv_cols], wv_sem.at[i])

    def cache_copies(b, slot):
        gs = pl.ds(y * groups, groups)
        return (pltpu.make_async_copy(kc_ref.at[b, gs], k_buf.at[slot], k_sem.at[slot]),
                pltpu.make_async_copy(vc_ref.at[b, gs], v_buf.at[slot], v_sem.at[slot]))

    reads = [(copies["x", i], copies["q", i]) for i in range(CHUNK_K)] + [(copies["k", i], copies["v", i]) for i in range(CHUNK_K)]
    reads += [cache_copies(b, b) for b in range(SLOTS)]

    def read_next(n):
        for pair in reads[:n]:
            for copy in pair:
                copy.start()
        del reads[:n]

    read_next(AHEAD)
    for i in range(CHUNK_K):
        ks = pl.ds(i * kc, kc)
        copies["x", i].wait()
        copies["q", i].wait()
        read_next(1)
        prod = jnp.dot(x_buf[:, ks], wq_buf[ks, :], preferred_element_type=jnp.float32)
        acc_q[...] = prod if i == 0 else acc_q[...] + prod
    q_send[...] = acc_q[...].astype(jnp.bfloat16).reshape(nm, rows, hl * head)
    pl.semaphore_wait(barrier, len(peers))
    for s in [4, 3, 5, 2, 6, 1, 7]:
        target = lax.rem(model + s, nm)
        remote(q_send.at[target], q_recv.at[model], sem_q.at[0, s], sem_q.at[1, nm - s], dev_m(target))
    q_recv[pl.ds(model, 1)] = q_send[pl.ds(model, 1)]

    mine = pl.ds(pl.multiple_of(model * rows, rows), rows)
    for i in range(CHUNK_K):
        ks = pl.ds(i * kc, kc)
        copies["k", i].wait()
        copies["v", i].wait()
        read_next(1)
        prod = jnp.dot(x_buf[mine, ks], wkv_buf[ks, :], preferred_element_type=jnp.float32)
        acc_kv[...] = prod if i == 0 else acc_kv[...] + prod
    kv_bf = acc_kv[...].astype(jnp.bfloat16)
    kv_send[...] = kv_bf
    kv_all[pl.ds(y, 1)] = kv_bf[None]
    for j in range(2 * groups):
        kv_rows[j] = kv_bf[:, j * head:(j + 1) * head].astype(jnp.float32)
    for s in (2, 1, 3):
        remote(kv_send, kv_all.at[y], sem_kv.at[0, s], sem_kv.at[1, ny - s], dev(y + s, x, core))

    my_cols = pl.ds(pl.multiple_of(core * cols, cols), cols)
    other_cols = pl.ds(pl.multiple_of((1 - core) * cols, cols), cols)
    my_rows = pl.ds(pl.multiple_of(core * depth, depth), depth)
    other_rows = pl.ds(pl.multiple_of((1 - core) * depth, depth), depth)
    own_w = pltpu.make_async_copy(wo_ref.at[:, my_cols], w_buf.at[my_rows], w_sem.at[2])
    own_w.start()
    remote(wo_ref.at[:, other_cols], w_buf.at[my_rows], w_sem.at[0], w_sem.at[1], partner)

    read_next(len(reads))
    for s in range(1, nm):
        arrive(q_recv.at[lax.rem(model + s, nm)], sem_q.at[1, s])
    for src in range(nm):
        for j in range(hl):
            q_rows[pl.ds(src * hl + j, rows, stride=heads), :] = q_recv[src, :, j * head:(j + 1) * head].astype(jnp.float32)

    scale = head ** -0.5
    hc = heads // nx

    def attend(k):
        def step(n, carry):
            positions = lax.broadcasted_iota(jnp.int32, (per_group, context), 1)
            pairs, scores, news = [], [], []
            for u in range(SEQS):
                b = k * r + n * SEQS + u
                slot = lax.rem(b, SLOTS)
                for copy in cache_copies(b, slot):
                    copy.wait()
                length = len_ref[b]
                for g in range(groups):
                    q = q_rows[pl.ds(pl.multiple_of(b * heads + g * per_group, per_group), per_group), :]
                    s = lax.dot_general(q.astype(jnp.bfloat16), k_buf[slot, g], (((1,), (1,)), ((), ())), preferred_element_type=jnp.float32) * scale
                    s = jnp.where(positions < length, s, -jnp.inf)
                    s_new = jnp.sum(q * kv_rows[g, pl.ds(b, 1), :], axis=1, keepdims=True) * scale
                    pairs.append((b, slot, g))
                    scores.append(s)
                    news.append(s_new)
            tops = [jnp.maximum(jnp.max(s, axis=1, keepdims=True), s_new) for s, s_new in zip(scores, news)]
            weights = [jnp.exp(s - m) for s, m in zip(scores, tops)]
            weight_news = [jnp.exp(s_new - m) for s_new, m in zip(news, tops)]
            sums = [jnp.sum(e, axis=1, keepdims=True) + e_new for e, e_new in zip(weights, weight_news)]
            for (b, slot, g), e, e_new, l in zip(pairs, weights, weight_news, sums):
                out = jnp.dot(e.astype(jnp.bfloat16), v_buf[slot, g], preferred_element_type=jnp.float32)
                out = out + e_new.astype(jnp.bfloat16).astype(jnp.float32) * kv_rows[groups + g, pl.ds(b, 1), :]
                o_rows[pl.ds(pl.multiple_of(b * heads + g * per_group, per_group), per_group), :] = out / l
            if (k + 1) * r + SLOTS <= rows:
                for u in range(SEQS):
                    b = k * r + n * SEQS + u
                    for copy in cache_copies(b + SLOTS, lax.rem(b, SLOTS)):
                        copy.start()
            return carry

        lax.fori_loop(0, r // SEQS, step, 0)
        for h in range(heads):
            o_send[k, h // hc, :, (h % hc) * head:(h % hc + 1) * head] = o_rows[pl.ds(k * r * heads + h, r, stride=heads), :].astype(jnp.bfloat16)
        for s in [4, 3, 5, 2, 6, 1, 7]:
            target = lax.rem(model + s, nm)
            remote(o_send.at[k, lax.div(target, 2)], o_all.at[k, model], sem_o.at[k, 0, s], sem_o.at[k, 1, nm - s], dev_m(target))
        o_all[k, pl.ds(model, 1)] = o_send[k, pl.ds(x, 1)]

    pos1 = (x, y)
    pos2 = (y, x)
    nexts = ((x_next, y_next), (y_next, x_next))
    prevs = ((x_prev, y_prev), (y_prev, x_prev))

    def cols_of(h, d):
        return pl.ds(pl.multiple_of(h * half + lax.rem(d + 4, 4) * block, block), block)

    def compute(k, h, d):
        lhs = o_all[k].reshape(nm * r, o_all.shape[3])
        acc = jnp.dot(lhs, w_buf[:, cols_of(h, d)], preferred_element_type=jnp.float32)
        part[:, k * r:(k + 1) * r, cols_of(h, d)] = acc.reshape(nm, r, block)

    low, high = pl.ds(0, hg), pl.ds(hg, hg)

    def send1(k, h, i, mi, d, target):
        kr = pl.ds(k * r, r)
        remote(part.at[mi, kr, cols_of(h, d)], recv1.at[h, i, :, kr, :], sems1.at[k, h, 0, i], sems1.at[k, h, 1, i], target)

    def wait1(k, h, i):
        arrive(recv1.at[h, i, :, pl.ds(k * r, r), :], sems1.at[k, h, 1, i])

    def s0(k):
        for s in range(1, nm):
            arrive(o_all.at[k, lax.rem(model + s, nm)], sem_o.at[k, 1, s])
        if k == 0:
            own_w.wait()
            arrive(w_buf.at[other_rows], w_sem.at[1])
        for h in range(2):
            p = pos1[h]
            compute(k, h, p + 2)
            send1(k, h, 0, low, p + 2, nexts[h][0])
            send1(k, h, 1, high, p + 2, prevs[h][0])
        for h in range(2):
            p = pos1[h]
            compute(k, h, p + 1)
            send1(k, h, 2, high, p + 1, nexts[h][0])
            compute(k, h, p - 1)
            send1(k, h, 3, low, p - 1, prevs[h][0])
        for h in range(2):
            compute(k, h, pos1[h])

    def s1(k):
        ks = slice(k * r, (k + 1) * r)
        for h in range(2):
            p = pos1[h]
            c = cols_of(h, p + 1)
            wait1(k, h, 0)
            part[0:hg, ks, c] = part[0:hg, ks, c] + recv1[h, 0, :, ks, :]
            send1(k, h, 4, low, p + 1, nexts[h][0])
            c = cols_of(h, p - 1)
            wait1(k, h, 1)
            part[hg:nm, ks, c] = part[hg:nm, ks, c] + recv1[h, 1, :, ks, :]
            send1(k, h, 5, high, p - 1, prevs[h][0])

    def send2(h, i, mi, target):
        remote(part.at[mi, :, cols_of(h, pos1[h])], recv2.at[h, i], sems2.at[h, 0, i], sems2.at[h, 1, i], target)

    def wait2(h, i):
        arrive(recv2.at[h, i], sems2.at[h, 1, i])

    def around(q):
        return lax.rem(q + 2, 4), lax.rem(q + 1, 4), lax.rem(q + 3, 4)

    def s2():
        for h in range(2):
            c = cols_of(h, pos1[h])
            far, up, down = around(pos2[h])
            for k in range(CHUNKS):
                for i in (2, 3, 4, 5):
                    wait1(k, h, i)
            part[0:hg, :, c] = part[0:hg, :, c] + recv1[h, 3] + recv1[h, 4]
            part[hg:nm, :, c] = part[hg:nm, :, c] + recv1[h, 2] + recv1[h, 5]
            send2(h, 0, 2 * far, nexts[h][1])
            send2(h, 1, 2 * far + 1, prevs[h][1])
            send2(h, 2, 2 * up + 1, nexts[h][1])
            send2(h, 3, 2 * down, prevs[h][1])

    def s3():
        for h in range(2):
            c = cols_of(h, pos1[h])
            far, up, down = around(pos2[h])
            wait2(h, 0)
            part[2 * up, :, c] = part[2 * up, :, c] + recv2[h, 0]
            send2(h, 4, 2 * up, nexts[h][1])
            wait2(h, 1)
            part[2 * down + 1, :, c] = part[2 * down + 1, :, c] + recv2[h, 1]
            send2(h, 5, 2 * down + 1, prevs[h][1])

    def region(h, j, d, sub=None, cc=None):
        c0 = pl.multiple_of((core if cc is None else cc) * cols + h * half + lax.rem(d + 4, 4) * block, block)
        j = lax.rem(j + 4, 4)
        mi = pl.ds(2 * j, 2) if sub is None else pl.ds(2 * j + sub, 1)
        return out_ref.at[mi, :, pl.ds(c0, block)]

    def push(reg, sems, index, target):
        remote(reg, reg, sems.at[(0,) + index], sems.at[(1,) + index], target)

    def pulled(reg, sems, index):
        arrive(reg, sems.at[(1,) + index])

    def spread(h, n, j):
        p = pos1[h]
        push(region(h, j, p), sems4, (h, n, 0), nexts[h][0])
        push(region(h, j, p), sems4, (h, n, 1), prevs[h][0])
        push(region(h, j, p), sems_d, (h, n, 0), partner)

    def relay(h, n, j):
        p = pos1[h]
        pulled(region(h, j, p - 1), sems4, (h, n, 0))
        push(region(h, j, p - 1, 0), sems4, (h, n, 2), nexts[h][0])
        push(region(h, j, p - 1), sems_d, (h, n, 1), partner)
        pulled(region(h, j, p + 1), sems4, (h, n, 1))
        push(region(h, j, p + 1, 1), sems4, (h, n, 3), prevs[h][0])
        push(region(h, j, p + 1), sems_d, (h, n, 2), partner)

    def finish(h, n, j):
        p = pos1[h]
        for sub in range(2):
            reg = region(h, j, p + 2, sub)
            pulled(reg, sems4, (h, n, 2 + sub))
            push(reg, sems_d, (h, n, 3 + sub), partner)

    def s4():
        for h in range(2):
            p, q = pos1[h], pos2[h]
            c = cols_of(h, p)
            for i in (2, 3, 4, 5):
                wait2(h, i)
            oc = pl.ds(pl.multiple_of(core * cols + h * half + p * block, block), block)
            for sub, plain, summed in ((0, 3, 4), (1, 2, 5)):
                mi = 2 * q + sub
                total = part[mi, :, c] + recv2[h, plain] + recv2[h, summed]
                total = x_buf[pl.ds(pl.multiple_of(mi * rows, rows), rows), oc].astype(jnp.float32) + total
                out_ref[mi, :, oc] = total.astype(out_ref.dtype)
            push(region(h, q, p), sems3, (h, 0), nexts[h][1])
            push(region(h, q, p), sems3, (h, 1), prevs[h][1])
        for h in range(2):
            spread(h, 0, pos2[h])

    def s5():
        for h in range(2):
            p, q = pos1[h], pos2[h]
            pulled(region(h, q - 1, p), sems3, (h, 0))
            push(region(h, q - 1, p, 0), sems3, (h, 2), nexts[h][1])
            pulled(region(h, q + 1, p), sems3, (h, 1))
            push(region(h, q + 1, p, 1), sems3, (h, 3), prevs[h][1])
        for h in range(2):
            spread(h, 1, pos2[h] - 1)
            spread(h, 2, pos2[h] + 1)

    def s6():
        for h in range(2):
            relay(h, 0, pos2[h])
        for h in range(2):
            p, q = pos1[h], pos2[h]
            pulled(region(h, q + 2, p, 0), sems3, (h, 2))
            pulled(region(h, q + 2, p, 1), sems3, (h, 3))
            spread(h, 3, q + 2)

    def s7():
        for h in range(2):
            relay(h, 1, pos2[h] - 1)
            relay(h, 2, pos2[h] + 1)
        for h in range(2):
            finish(h, 0, pos2[h])
        for h in range(2):
            relay(h, 3, pos2[h] + 2)
        for n, d in ((1, -1), (2, 1), (3, 2)):
            for h in range(2):
                finish(h, n, pos2[h] + d)

    def new_rows():
        for s in range(1, ny):
            arrive(kv_all.at[lax.rem(y + s, ny)], sem_kv.at[1, s])
        kv_heads = ny * groups
        for half_, ref in ((0, kn_ref), (1, vn_ref)):
            for g in range(kv_heads):
                c0 = half_ * kv_cols + (g % groups) * head
                kn_rows[half_, pl.ds(g, rows, stride=kv_heads), :] = kv_all[g // groups, :, c0:c0 + head].astype(jnp.float32)
            ref[...] = kn_rows[half_].reshape(rows, kv_heads, head).astype(jnp.bfloat16)

    attend(0)
    attend(1)
    s0(0)
    attend(2)
    s0(1)
    s1(0)
    attend(3)
    s0(2)
    s1(1)
    s0(3)
    s1(2)
    s1(3)
    s2()
    s3()
    s4()
    new_rows()
    s5()
    s6()
    s7()
    for h in range(2):
        p, q = pos1[h], pos2[h]
        for n, d in ((0, 0), (1, -1), (2, 1), (3, 2)):
            for i, (dp, sub) in enumerate(((0, None), (-1, None), (1, None), (2, 0), (2, 1))):
                pulled(region(h, q + d, p + dp, sub, 1 - core), sems_d, (h, n, i))
    for copy in sends:
        copy.wait_send()


def layer(ny, nx, tokens, w_query, w_key, w_value, w_out, key_cache, value_cache, lengths):
    batch, width = tokens.shape
    rows, kv_heads, context, head = key_cache.shape
    nm = 2 * nx
    groups = kv_heads // ny
    kv_cols = groups * head
    heads = nm * w_query.shape[1] // head
    depth = w_out.shape[0]
    block = width // 16
    r = rows // CHUNKS
    hbm_spec = pl.BlockSpec(memory_space=pltpu.HBM)
    vmem_spec = pl.BlockSpec(memory_space=pltpu.VMEM)
    dma = pltpu.SemaphoreType.DMA
    bf, f32 = jnp.bfloat16, jnp.float32
    new_shape = jax.ShapeDtypeStruct((rows, kv_heads, head), bf)
    return pl.pallas_call(
        functools.partial(layer_kernel, ny, nx),
        out_shape=(jax.ShapeDtypeStruct((nm, rows, width), bf), new_shape, new_shape),
        in_specs=[hbm_spec] * 7 + [pl.BlockSpec(memory_space=pltpu.SMEM)],
        out_specs=(vmem_spec,) * 3,
        scratch_shapes=[
            pltpu.VMEM((batch, width), bf), pltpu.VMEM(w_query.shape, bf), pltpu.VMEM((width, 2 * kv_cols), bf),
            pltpu.VMEM((batch, w_query.shape[1]), f32), pltpu.VMEM((rows, 2 * kv_cols), f32),
            pltpu.VMEM((nm, rows, w_query.shape[1]), bf), pltpu.VMEM((nm, rows, w_query.shape[1]), bf),
            pltpu.VMEM((rows * heads, head), f32),
            pltpu.VMEM((rows, 2 * kv_cols), bf), pltpu.VMEM((ny, rows, 2 * kv_cols), bf), pltpu.VMEM((2 * groups, rows, head), f32),
            pltpu.VMEM((2, rows * kv_heads, head), f32), pltpu.VMEM((rows * heads, head), f32),
            pltpu.VMEM((SLOTS, groups, context, head), bf), pltpu.VMEM((SLOTS, groups, context, head), bf),
            pltpu.VMEM((2 * depth, width // 2), bf),
            pltpu.VMEM((CHUNKS, nx, r, 2 * depth), bf), pltpu.VMEM((CHUNKS, nm, r, 2 * depth), bf),
            pltpu.VMEM((nm, rows, width // 2), f32),
            pltpu.VMEM((2, 6, nm // 2, rows, block), f32),
            pltpu.VMEM((2, 6, rows, block), f32),
            dma((CHUNK_K,)), dma((CHUNK_K,)), dma((CHUNK_K,)), dma((CHUNK_K,)), dma((SLOTS,)), dma((SLOTS,)), dma((3,)),
            dma((2, nm)), dma((2, ny)), dma((CHUNKS, 2, nm)), dma((CHUNKS, 2, 2, 6)), dma((2, 2, 6)), dma((2, 2, 4)),
            dma((2, 2, 4, 4)), dma((2, 2, 4, 5)),
        ],
        compiler_params=pltpu.CompilerParams(collective_id=5, has_side_effects=True, vmem_limit_bytes=47 * 1024 * 1024),
        name="layer",
    )(tokens, w_query, w_key, w_value, w_out, key_cache, value_cache, lengths)


def solution(mesh):
    heads_count = mesh.shape["heads"]
    chips = mesh.shape["model"] // 2

    def local_step(tokens, w_query, w_key, w_value, w_out, key_cache, value_cache, lengths):
        out, key_new, value_new = layer(heads_count, chips, tokens, w_query, w_key, w_value, w_out, key_cache, value_cache, lengths)
        return (out.reshape(tokens.shape), key_new, value_new)

    cache_spec = P(("replica", "model"), None, None, None)
    new_spec = P(("replica", "model"), None, None)
    return jax.shard_map(
        local_step,
        mesh=mesh,
        in_specs=(P("replica", None), P(None, ("heads", "model")), P(None, None), P(None, None), P(("heads", "model"), None), cache_spec, cache_spec, P(("replica", "model"))),
        out_specs=(P("replica", None), new_spec, new_spec),
        check_vma=False,
    )
```
